32 devices in a mesh: grp: 4 (over y, core), blk: 8 (over z, x).
Axes of the slice: x: 2, y: 2, z: 4, core: 2. Of those that a mesh axis runs over, the one named last changes fastest.
Arguments:
- embeds: bfloat16 [4, 8192, 1024], P('grp', 'blk')
- doc_ids: int32 [4, 8192], P('grp', 'blk'), may hold values from 0 to 8191, each once within a row
- prior_max: float32 [4, 8192], P('grp', 'blk'), may hold values from -0.2 to 0.6
- owned: bfloat16 [2048, 1024], P(('grp', 'blk')), may hold values from -6 to 6
- owned_ids: int32 [2048], P(('grp', 'blk')), may hold values from 0 to 2047, each once
- owner_dest: int32 [2048, 1], P(('grp', 'blk')), may hold values from 0 to 31; in each aligned block of 64 rows (0 to 63, 64 to 127, ...) at most 4 rows name the same one
Outputs:
- running_max: float32 [4, 8192], P('grp', 'blk')
- next_rows: bfloat16 [4096, 1024], P(('grp', 'blk'))
- next_ids: int32 [4096], P(('grp', 'blk'))
The draws below stay inside these ranges and needn't reach their ends.
Inputs may be any that keep to these rules, and one draw needn't show every extreme that they name: `owner_dest`: among the 64 rows of one device no target is named more than 4 times, a bound that some block reaches.
All inputs are finite; a program needn't handle non-finite values.
Results may differ from the reference program's by a relative error of at most 0.0016.
Values may be sent and summed in bfloat16 or wider, within the bound.
A program may use at most 64 MiB of HBM per device.

```python
import math
import jax
import jax.numpy as jnp
import numpy as np
from jax import lax

E = 1024
ROWS_DEV = 1024
CYCLE = 3
CAP = 4
CR = 8192
OWN_DEV = 64
TOTAL_OWN = 2048
SLOTS = 128
N_GRP = 4
N_BLK = 8
DEVICES = 32


def draw_embeds(key, part):
    keys = jax.random.split(jax.random.fold_in(key, 7), 4)
    nblk = CR // ROWS_DEV
    base = jax.random.normal(keys[0], (N_GRP, CR, E), jnp.float32)
    offset = jax.random.randint(keys[1], (N_GRP, CR), 0, CYCLE + 1)
    within = jax.random.randint(keys[2], (N_GRP, CR), 0, ROWS_DEV)
    blocks = jnp.arange(CR, dtype=jnp.int32)[None, :] // ROWS_DEV
    partner = (blocks - offset) % nblk * ROWS_DEV + within
    partner_rows = jnp.take_along_axis(base, partner[:, :, None], axis=1)
    weight = jnp.exp(jax.random.uniform(keys[3], (N_GRP, CR, 1), jnp.float32, jnp.log(0.3), jnp.log(3.0)))
    result = base + weight * partner_rows
    return result.astype(jnp.bfloat16)


def levels(own_key, shape, pieces, smallest, high):
    def one(dim, blocks):
        draws = jax.random.uniform(jax.random.fold_in(jax.random.fold_in(own_key, 6), dim), (blocks,), jnp.float32, smallest / len(pieces), high / len(pieces))
        return jnp.repeat(jnp.exp(draws), shape[dim] // blocks).reshape((-1,) + (1,) * (len(shape) - dim - 1))

    gain = one(*pieces[0])
    for cut in pieces[1:]:
        gain = gain * one(*cut)
    return gain


def deal_out(key, own, number, rows, number_of, top, limit, lean):
    order = jax.random.permutation(key, number_of)
    heavy_load, ordinary = load_shares(number_of, rows * top, limit, lean, True), load_shares(number_of, rows * top, limit, lean, False)
    places = jnp.arange(number_of)

    def named(sizes, turn):
        used = int((sizes > 0).sum())
        fixed = max(1, used // 4)
        moved = fixed + (places - fixed + turn * (used - fixed)) % max(1, number_of - fixed)
        return jnp.zeros((number_of,), jnp.int32).at[order[jnp.where(places < fixed, places, moved)]].set(jnp.asarray(sizes, jnp.int32))

    sizes = jnp.where(number % 4 == 0, named(heavy_load, number // 4), named(ordinary, number - number // 4 - 1))
    mixed = jax.random.permutation(jax.random.fold_in(own, 3), number_of)
    giver, taker = mixed[0:number_of // 2 * 2:2], mixed[1:number_of // 2 * 2:2]
    room = jnp.minimum(sizes[giver] - 1, limit - sizes[taker]) // 2
    room = jnp.where((giver == order[0]) | (taker == order[0]) | (sizes[taker] == 0), 0, jnp.maximum(room, 0))
    moved = jax.random.randint(jax.random.fold_in(own, 4), (number_of // 2,), 0, 1 << 20) % (room + 1)
    sizes = sizes.at[giver].add(-moved).at[taker].add(moved)
    items = jnp.searchsorted(jnp.cumsum(sizes), jnp.arange(rows * top), side="right").astype(jnp.int32)
    grid = items.reshape(top, rows).T
    grid = grid[jax.random.permutation(jax.random.fold_in(own, 1), rows)]
    turn = jax.random.randint(jax.random.fold_in(own, 2), (rows, 1), 0, top)
    return jnp.take_along_axis(grid, (jnp.arange(top)[None, :] + turn) % top, axis=1)


def load_shares(number_of, total, reach, skew, full):
    loads = [(1 << 20) // math.isqrt(standing ** skew) + 1 for standing in range(1, number_of + 1)]
    largest = reach if full else min(reach, max(-(-total // number_of), total * loads[0] // sum(loads)))
    least = 1 if total - largest >= number_of - 1 else 0
    given, surplus = [largest] + [least] * (number_of - 1), total - largest - least * (number_of - 1)
    while surplus > 0:
        free = [i for i in range(1, number_of) if given[i] < largest] or [i for i in range(1, number_of) if given[i] < reach]
        mass, left = sum([loads[i] for i in free]), surplus
        for i in free:
            addition = min(reach - given[i], max(1, left * loads[i] // mass), surplus)
            given[i] = given[i] + addition
            surplus = surplus - addition
    return np.array(given)


def noise(key, extent, spread, bound, cuts=(), held_as=jnp.bfloat16):
    gain = levels(key, extent, cuts, -0.22, 0.18) if cuts else 1.0
    array = jax.random.normal(key, extent, jnp.float32) * spread * gain
    return jnp.minimum(jnp.maximum(array, -bound), bound).astype(held_as)


def setup_inputs(seed: int = 0) -> dict:
    key_list = jax.random.split(jax.random.key(seed), 7)
    embeds = draw_embeds(jax.random.fold_in(key_list[6], 71), 0)
    doc_ids = jax.vmap(lambda own: jax.random.permutation(own, CR))(jax.random.split(key_list[1], N_GRP)).reshape((N_GRP, CR)).astype(jnp.int32)
    prior_max = jnp.clip(-0.2 + 0.8 * jax.random.uniform(key_list[2], (N_GRP, CR), jnp.float32) ** levels(key_list[2], (N_GRP, CR), ((0, 4), (1, 8)), -0.2, 0.2), -0.2, 0.6)
    owned = noise(key_list[3], (TOTAL_OWN, E), 1.0, 6.0, ((0, 32),))
    owned_ids = jax.random.permutation(key_list[4], TOTAL_OWN).astype(jnp.int32)
    owner_dest_keys = jax.random.split(jax.random.fold_in(key_list[5], 1), TOTAL_OWN // OWN_DEV)
    owner_dest_turns = jax.random.permutation(jax.random.fold_in(key_list[5], 3), TOTAL_OWN // OWN_DEV)
    owner_dest = jax.vmap(lambda own, number: deal_out(jax.random.fold_in(key_list[5], 2), own, number, OWN_DEV, DEVICES, 1, CAP, 2))(owner_dest_keys, owner_dest_turns).reshape((TOTAL_OWN, 1))
    return {"embeds": embeds, "doc_ids": doc_ids, "prior_max": prior_max, "owned": owned, "owned_ids": owned_ids, "owner_dest": owner_dest}


def normalize(matrix):
    values = matrix.astype(jnp.float32)
    scale = lax.rsqrt(lax.optimization_barrier(jnp.sum(values * values, axis=-1, keepdims=True)) + 1e-06)
    return (values * scale).astype(jnp.bfloat16)

def tile_max(operands):
    row_normed, row_ids, col_normed, col_ids = operands
    scores = lax.dot_general(row_normed, col_normed, (((1,), (1,)), ((), ())), preferred_element_type=jnp.float32)
    masked = jnp.where(col_ids[None, :] < row_ids[:, None], scores, jnp.float32(-2.0))
    return lax.optimization_barrier(jnp.max(masked, axis=1))

def reference(embeds, doc_ids, prior_max, owned, owned_ids, owner_dest):
    normed = normalize(embeds).reshape(N_GRP, N_BLK, ROWS_DEV, E)
    numbers = doc_ids.reshape(N_GRP, N_BLK, ROWS_DEV)
    running = prior_max.reshape(N_GRP, N_BLK, ROWS_DEV).astype(jnp.float32)
    for distance in range(CYCLE + 1):
        col_normed = jnp.roll(normed, distance, axis=1)
        col_ids = jnp.roll(numbers, distance, axis=1)
        found = lax.map(tile_max, (normed.reshape(-1, ROWS_DEV, E), numbers.reshape(-1, ROWS_DEV), col_normed.reshape(-1, ROWS_DEV, E), col_ids.reshape(-1, ROWS_DEV)))
        running = jnp.maximum(running, found.reshape(N_GRP, N_BLK, ROWS_DEV))
    running_max = running.reshape(N_GRP, CR)
    devices = N_GRP * N_BLK
    owned_normed = normalize(owned)
    target = owner_dest[:, 0].astype(jnp.int32)
    grouped = target.reshape(devices, OWN_DEV)
    onehot = (grouped[:, :, None] == jnp.arange(devices, dtype=jnp.int32)[None, None, :]).astype(jnp.int32)
    position = lax.optimization_barrier(jnp.sum(jnp.cumsum(onehot, axis=1) * onehot, axis=2)) - 1
    source = jnp.arange(devices, dtype=jnp.int32)[:, None]
    place = (grouped * SLOTS + source * CAP + position).reshape(-1).astype(jnp.int32)
    next_rows = jnp.zeros((devices * SLOTS, E), jnp.bfloat16).at[place].set(owned_normed)
    next_ids = jnp.full((devices * SLOTS,), -1, jnp.int32).at[place].set(owned_ids.astype(jnp.int32))
    return (running_max, next_rows, next_ids)
```

```python
import functools

import jax
import jax.numpy as jnp
from jax import lax
from jax.experimental import pallas as pl
from jax.experimental.pallas import tpu as pltpu
from jax.sharding import PartitionSpec as P

CYCLE = 3
CAP = 4
CHUNKS = 4
LANES = 128
EMPTY = -2.0


def make_plan(nz):
    received = [[((z - 1) % nz, (z - 1) % nz), ((z - 2) % nz, (z - 1) % nz)] for z in range(nz)]
    late = [False] * nz
    own_to = [(-1, 0)] * nz
    forward = [[(-1, 0)] * len(received[z]) for z in range(nz)]
    rank = [[0] * len(received[z]) for z in range(nz)]
    returns = [0] * nz
    for z in range(nz):
        for slot, (block, source) in enumerate(received[z]):
            if block == source:
                own_to[source] = (z, slot)
            else:
                held = [entry[0] for entry in received[source]].index(block)
                forward[source][held] = (z, slot)
            rank[z][slot] = returns[block]
            returns[block] += 1
    return received, own_to, late, forward, rank, returns


def pick(index, values):
    result = jnp.int32(values[0])
    for i in range(1, len(values)):
        if values[i] != values[0]:
            result = jnp.where(index == i, jnp.int32(values[i]), result)
    return result


def ring_kernel(plan, sizes, emb, ids, prior, owned, owned_ids, dest,
           run_out, rows_out, ids_out,
           raw, nrm, idv, idt, acc, ret, obuf, oid,
           local_sem, send_sem, recv_sem, ids_send, ids_recv, ret_send, ret_recv,
           rows_send, rows_recv, oids_send, oids_recv, keep_sem):
    n_grp, n_blk = sizes
    devices = n_grp * n_blk
    nz = n_blk // 2
    received, own_to, late, forward, rank, returns = plan
    slots = max(len(entry) for entry in received)
    rows = emb.shape[1]
    ch = rows // CHUNKS
    g = lax.axis_index("grp")
    b = lax.axis_index("blk")
    flip = g % 2
    z = b // 2
    x = b % 2
    role = z + flip * (nz - 1 - 2 * z)

    def block_of(zr):
        return 2 * (zr + flip * (nz - 1 - 2 * zr)) + x

    partner = b + 1 - 2 * x

    def table(values, slot=None, empty=0):
        if slot is None:
            return pick(role, values)
        return pick(role, [v[slot] if slot < len(v) else empty for v in values])

    own_z, own_slot = table([v[0] for v in own_to]), table([v[1] for v in own_to])
    is_late = table([int(v) for v in late])
    exists = [table([[1] * len(v) for v in received], s) for s in range(slots)]
    slot_z = [table([[e[0] for e in v] for v in received], s) for s in range(slots)]
    fwd_z = [table([[e[0] for e in v] for v in forward], s, -1) for s in range(slots)]
    fwd_slot = [table([[e[1] for e in v] for v in forward], s) for s in range(slots)]
    ranks = [table(rank, s) for s in range(slots)]
    n_returns = table(returns)
    blocks = [b, partner] + [block_of(slot_z[s]) for s in range(slots)]

    def span(c):
        if isinstance(c, int):
            return pl.ds(c * ch, ch)
        return pl.ds(pl.multiple_of(c * ch, ch), ch)

    def remote(src, dst, ssem, rsem, blk, grp=None):
        return pltpu.make_async_remote_copy(
            src_ref=src, dst_ref=dst, send_sem=ssem, recv_sem=rsem,
            device_id=(g if grp is None else grp, blk), device_id_type=pl.DeviceIdType.MESH)

    def chunk_copy(src, lane, to_slot, blk, c):
        return remote(src, raw.at[to_slot, span(c), :], send_sem.at[lane, c], recv_sem.at[to_slot, c], blk)

    def ids_copy(src, lane, to_slot, blk):
        return remote(src, idv.at[to_slot], ids_send.at[lane], ids_recv.at[to_slot], blk)

    def own_column(c):
        return chunk_copy(emb.at[0, span(c), :], 1, 2 + own_slot, block_of(own_z), c)

    def partner_copy(c):
        return chunk_copy(emb.at[0, span(c), :], 0, 1, partner, c)

    def forward_copy(s, c):
        return chunk_copy(raw.at[2 + s, span(c), :], 2 + s, 2 + fwd_slot[s], block_of(fwd_z[s]), c)

    def start_own_column():
        ids_copy(ids, 1, 2 + own_slot, block_of(own_z)).start()
        for c in range(CHUNKS):
            own_column(c).start()

    local = pltpu.make_async_copy(emb.at[0], raw.at[0], local_sem)
    local.start()

    @pl.when((own_z >= 0) & (is_late == 0))
    def _():
        start_own_column()

    ids_copy(ids, 0, 1, partner).start()
    for c in range(CHUNKS):
        partner_copy(c).start()

    def normalize(values):
        values = values.astype(jnp.float32)
        scale = lax.rsqrt(jnp.sum(values * values, axis=-1, keepdims=True) + 1e-06)
        return (values * scale).astype(jnp.bfloat16)

    own_dev = owned.shape[0]
    owned_normed = normalize(owned[...])
    t_col = dest[...].astype(jnp.float32)
    t_row = jnp.transpose(jnp.broadcast_to(t_col, (own_dev, LANES)))[0:1, :]
    row_i = lax.broadcasted_iota(jnp.int32, (own_dev, own_dev), 0)
    col_i = lax.broadcasted_iota(jnp.int32, (own_dev, own_dev), 1)
    earlier = jnp.where((row_i < col_i) & (t_col == t_row), 1.0, 0.0)
    position = jnp.sum(earlier, axis=0, keepdims=True)
    place = t_row * CAP + position
    which = lax.broadcasted_iota(jnp.int32, (devices * CAP, own_dev), 0).astype(jnp.float32)
    onehot = jnp.where(which == place, 1.0, 0.0).astype(jnp.bfloat16)
    outgoing = jnp.dot(onehot, owned_normed, preferred_element_type=jnp.float32).astype(jnp.bfloat16)
    dev_i = lax.broadcasted_iota(jnp.int32, (devices, own_dev), 0).astype(jnp.float32)
    lane_i = lax.broadcasted_iota(jnp.int32, (devices, LANES), 1)
    number = owned_ids[...].astype(jnp.float32) + 1.0
    outgoing_ids = jnp.full((devices, LANES), -1.0, jnp.float32)
    for k in range(CAP):
        here = jnp.where((dev_i == t_row) & (position == float(k)), number, 0.0)
        found = jnp.sum(here, axis=1, keepdims=True) - 1.0
        outgoing_ids = jnp.where(lane_i % CAP == k, found, outgoing_ids)
    outgoing_ids = outgoing_ids.astype(jnp.int32)
    for d in range(devices):
        obuf[d] = outgoing[d * CAP:(d + 1) * CAP, :]
        oid[d] = outgoing_ids[d:d + 1, :]

    def ready(s, c):
        at = span(c)
        nrm[s, at, :] = normalize(raw[s, at, :])
        for p in range(ch // LANES):
            at = pl.ds(pl.multiple_of(c * ch + p * LANES, LANES), LANES)
            line = idv[s, :, at].astype(jnp.float32)
            idt[s, at, :] = jnp.transpose(jnp.broadcast_to(line, (LANES, LANES)))

    def tile(row, row_at, width, col, col_at):
        scores = lax.dot_general(
            nrm[col, col_at, :], nrm[row, row_at, :], (((1,), (1,)), ((), ())),
            preferred_element_type=jnp.float32)
        row_ids = idv[row, :, row_at].astype(jnp.float32)
        col_ids = idt[col, col_at, :]
        parts = []
        for p in range(width // LANES):
            cut = slice(p * LANES, (p + 1) * LANES)
            masked = jnp.where(col_ids < row_ids[:, cut], scores[:, cut], EMPTY)
            parts.append(jnp.max(masked, axis=0, keepdims=True))
        acc[row, :, row_at] = jnp.maximum(acc[row, :, row_at], jnp.concatenate(parts, axis=1))

    whole = pl.ds(0, rows)

    acc[0] = prior[...]
    for s in range(1, 2 + slots):
        acc[s] = jnp.full((1, rows), EMPTY, jnp.float32)
    idv[0] = ids[...]
    local.wait()

    @pl.loop(0, CHUNKS)
    def _(c):
        ready(0, c)

    me = g * n_blk + b

    def to_device(step):
        other = (me + step) % devices
        return other, other // n_blk, other % n_blk

    @pl.loop(1, devices)
    def _(step):
        other, og, ob = to_device(step)
        remote(obuf.at[other], rows_out.at[me], rows_send, rows_recv, ob, og).start()
        remote(oid.at[other], ids_out.at[me], oids_send, oids_recv, ob, og).start()

    keep_rows = pltpu.make_async_copy(obuf.at[me], rows_out.at[me], keep_sem.at[0])
    keep_ids = pltpu.make_async_copy(oid.at[me], ids_out.at[me], keep_sem.at[1])
    keep_rows.start()
    keep_ids.start()

    def is_row(u, v):
        diff = (u - v + n_blk) % n_blk
        return (diff >= 1) & (diff <= CYCLE)

    def against_whole(s, c, other):
        @pl.when(is_row(blocks[s], blocks[other]))
        def _():
            tile(s, span(c), ch, other, whole)

        @pl.when(is_row(blocks[other], blocks[s]))
        def _():
            tile(other, whole, rows, s, span(c))

    def against_part(s, c, other, count):
        @pl.when(is_row(blocks[s], blocks[other]))
        def _():
            @pl.loop(0, count)
            def _(j):
                tile(s, span(c), ch, other, span(j))

        @pl.when(is_row(blocks[other], blocks[s]))
        def _():
            @pl.loop(0, count)
            def _(j):
                tile(other, span(j), ch, s, span(c))

    def arrive(s, c):
        chunk_copy(raw.at[s, span(c), :], 0, s, partner, c).wait_recv()

        @pl.when(c == 0)
        def _():
            ids_copy(idv.at[s], 0, s, partner).wait_recv()

        if s >= 2:
            @pl.when(fwd_z[s - 2] >= 0)
            def _():
                forward_copy(s - 2, c).start()

                @pl.when(c == 0)
                def _():
                    ids_copy(idv.at[s], s, 2 + fwd_slot[s - 2], block_of(fwd_z[s - 2])).start()

    @pl.loop(0, CHUNKS)
    def _(c):
        tile(0, whole, rows, 0, span(c))

    @pl.loop(0, CHUNKS)
    def _(c):
        @pl.when(exists[0] == 1)
        def _():
            arrive(2, c)
            ready(2, c)
            against_whole(2, c, 0)

    @pl.when((own_z >= 0) & (is_late == 1))
    def _():
        start_own_column()

    @pl.loop(0, CHUNKS)
    def _(c):
        for s in range(1, slots):
            @pl.when(exists[s] == 1)
            def _(s=s):
                arrive(2 + s, c)
                ready(2 + s, c)
                against_whole(2 + s, c, 0)
                against_part(2 + s, c, 1, c)

        arrive(1, c)
        ready(1, c)

        @pl.when(is_row(b, partner))
        def _():
            tile(0, whole, rows, 1, span(c))

        @pl.when(exists[0] == 1)
        def _():
            against_whole(1, c, 2)

        for s in range(1, slots):
            @pl.when(exists[s] == 1)
            def _(s=s):
                against_part(1, c, 2 + s, c + 1)

    back = remote(acc.at[1], ret.at[0], ret_send.at[0], ret_recv.at[0], partner)
    back.start()
    for s in range(slots):
        @pl.when(exists[s] == 1)
        def _(s=s):
            remote(acc.at[2 + s], ret.at[1 + ranks[s]], ret_send.at[1 + s], ret_recv.at[1 + ranks[s]],
                   block_of(slot_z[s])).start()

    for c in range(CHUNKS):
        partner_copy(c).wait_send()
    ids_copy(ids, 0, 1, partner).wait_send()

    @pl.when(own_z >= 0)
    def _():
        for c in range(CHUNKS):
            own_column(c).wait_send()
        ids_copy(ids, 1, 2 + own_slot, block_of(own_z)).wait_send()

    for s in range(slots):
        @pl.when(fwd_z[s] >= 0)
        def _(s=s):
            for c in range(CHUNKS):
                forward_copy(s, c).wait_send()
            ids_copy(idv.at[2 + s], 2 + s, 2 + fwd_slot[s], block_of(fwd_z[s])).wait_send()

    keep_rows.wait()
    keep_ids.wait()
    others = pl.ds(0, devices - 1)
    pltpu.make_async_copy(obuf.at[others], rows_out.at[others], rows_send).wait()
    pltpu.make_async_copy(oid.at[others], ids_out.at[others], oids_send).wait()
    pltpu.make_async_copy(obuf.at[others], rows_out.at[others], rows_recv).wait()
    pltpu.make_async_copy(oid.at[others], ids_out.at[others], oids_recv).wait()

    back.wait_recv()
    run_out[...] = jnp.maximum(acc[0], ret[0])
    for k in range(max(returns)):
        @pl.when(k < n_returns)
        def _(k=k):
            remote(acc.at[1], ret.at[1 + k], ret_send.at[0], ret_recv.at[1 + k], partner).wait_recv()
            run_out[...] = jnp.maximum(run_out[...], ret[1 + k])

    back.wait_send()
    for s in range(slots):
        @pl.when(exists[s] == 1)
        def _(s=s):
            remote(acc.at[2 + s], ret.at[1 + ranks[s]], ret_send.at[1 + s], ret_recv.at[1 + ranks[s]],
                   block_of(slot_z[s])).wait_send()


OWN, PAIR, ONE, ZERO, THREE = range(5)
SELF_UNIT = (OWN, OWN)
OWN_PAIR = (PAIR, OWN)
UNITS_FIRST = (
    ((SELF_UNIT,), ()),
    ((SELF_UNIT,), ()),
    ((SELF_UNIT,), ((ONE, PAIR), OWN_PAIR)),
    ((SELF_UNIT,), ((ONE, PAIR), OWN_PAIR)),
)
UNITS_SECOND = (
    ((), (OWN_PAIR,)),
    (((ZERO, OWN),), ((PAIR, ZERO), OWN_PAIR)),
    (((ONE, OWN),), ((ZERO, PAIR), (THREE, OWN), (THREE, PAIR))),
    ((), ((ZERO, OWN), (ZERO, PAIR))),
)


def line_kernel(sizes, emb, ids, prior, owned, owned_ids, dest,
                run_out, rows_out, ids_out,
                raw, nrm, idv, idt, acc, ret, obuf, oid, prior_v, owned_v, number_v, dest_v,
                local_sem, in_sem, send_sem, recv_sem, ids_send, ids_recv, ret_send, ret_recv,
                rows_send, rows_recv, oids_send, oids_recv, keep_sem):
    n_grp, n_blk = sizes
    devices = n_grp * n_blk
    rows = emb.shape[1]
    ch = rows // CHUNKS
    half = ch // 2
    g = lax.axis_index("grp")
    b = lax.axis_index("blk")
    flip = g % 2
    z = b // 2
    x = b % 2
    role = z + flip * (3 - 2 * z)
    partner = b + 1 - 2 * x
    me = g * n_blk + b

    def block_of(r):
        return 2 * (r + flip * (3 - 2 * r)) + x

    def to_device(step):
        other = (me + step) % devices
        return other, other // n_blk, other % n_blk

    barrier = pltpu.get_barrier_semaphore()

    @pl.loop(1, devices)
    def _(step):
        _, og, ob = to_device(step)
        pl.semaphore_signal(barrier, inc=1, device_id=(og, ob), device_id_type=pl.DeviceIdType.MESH)

    local = pltpu.make_async_copy(emb.at[0], raw.at[OWN], local_sem)
    local.start()
    inputs = [pltpu.make_async_copy(src, dst, in_sem.at[i]) for i, (src, dst) in enumerate((
        (ids, idv.at[OWN]), (prior, prior_v), (owned, owned_v), (owned_ids, number_v), (dest, dest_v)))]
    for copy in inputs:
        copy.start()

    pl.semaphore_wait(barrier, devices - 1)

    def remote(src, dst, ssem, rsem, blk, grp=None):
        return pltpu.make_async_remote_copy(
            src_ref=src, dst_ref=dst, send_sem=ssem, recv_sem=rsem,
            device_id=(g if grp is None else grp, blk), device_id_type=pl.DeviceIdType.MESH)

    def piece(k):
        if isinstance(k, int):
            return pl.ds(k * half, half)
        return pl.ds(pl.multiple_of(k * half, half), half)

    def span(c):
        return pl.ds(pl.multiple_of(c * ch, ch), ch)

    whole = pl.ds(0, rows)
    pieces = 2 * CHUNKS

    own_slot = pick(role, [ZERO, ONE, ONE, THREE])
    own_to = block_of(pick(role, [1, 2, 3, 2]))
    has_own = role != 2
    onward = block_of(role + 1)
    gives_pair = (role > 0) | (x == 0)
    takes_pair = (role > 0) | (x == 1)
    early = role >= 2

    def own_copy(k):
        return remote(emb.at[0, piece(k), :], raw.at[own_slot, piece(k), :],
                      send_sem.at[0, k], recv_sem.at[own_slot, k], own_to)

    def pair_copy(k):
        return remote(emb.at[0, piece(k), :], raw.at[PAIR, piece(k), :],
                      send_sem.at[1, k], recv_sem.at[PAIR, k], partner)

    def onward_copy(s, k):
        return remote(raw.at[s, piece(k), :], raw.at[s, piece(k), :],
                      send_sem.at[s, k], recv_sem.at[s, k], onward)

    def ids_copy(src, lane, slot, blk):
        return remote(src, idv.at[slot], ids_send.at[lane], ids_recv.at[slot], blk)

    @pl.when(has_own)
    def _():
        ids_copy(ids, 0, own_slot, own_to).start()

    @pl.when(role < 2)
    def _():
        for k in range(pieces):
            own_copy(k).start()

    @pl.when(gives_pair)
    def _():
        ids_copy(ids, 1, PAIR, partner).start()

    def start_pair():
        for k in range(pieces):
            pair_copy(k).start()

    @pl.when(early)
    def _():
        start_pair()

    def normalize(values):
        values = values.astype(jnp.float32)
        scale = lax.rsqrt(jnp.sum(values * values, axis=-1, keepdims=True) + 1e-06)
        return (values * scale).astype(jnp.bfloat16)

    def ready(s, c):
        at = span(c)
        nrm[s, at, :] = normalize(raw[s, at, :])
        for p in range(ch // LANES):
            at = pl.ds(pl.multiple_of(c * ch + p * LANES, LANES), LANES)
            line = idv[s, :, at].astype(jnp.float32)
            idt[s, at, :] = jnp.transpose(jnp.broadcast_to(line, (LANES, LANES)))

    def tile(row, row_at, width, col, col_at):
        scores = lax.dot_general(
            nrm[col, col_at, :], nrm[row, row_at, :], (((1,), (1,)), ((), ())),
            preferred_element_type=jnp.float32)
        row_ids = idv[row, :, row_at].astype(jnp.float32)
        col_ids = idt[col, col_at, :]
        parts = []
        for p in range(width // LANES):
            cut = slice(p * LANES, (p + 1) * LANES)
            masked = jnp.where(col_ids < row_ids[:, cut], scores[:, cut], EMPTY)
            parts.append(jnp.max(masked, axis=0, keepdims=True))
        acc[row, :, row_at] = jnp.maximum(acc[row, :, row_at], jnp.concatenate(parts, axis=1))

    for s in range(1, 5):
        acc[s] = jnp.full((1, rows), EMPTY, jnp.float32)
    for copy in inputs:
        copy.wait()
    acc[OWN] = prior_v[...]
    local.wait()

    @pl.loop(0, CHUNKS)
    def _(c):
        ready(OWN, c)

    own_dev = owned.shape[0]
    owned_normed = normalize(owned_v[...])
    t_col = dest_v[...].reshape(own_dev, 1).astype(jnp.float32)
    t_row = jnp.transpose(jnp.broadcast_to(t_col, (own_dev, LANES)))[0:1, :]
    row_i = lax.broadcasted_iota(jnp.int32, (own_dev, own_dev), 0)
    col_i = lax.broadcasted_iota(jnp.int32, (own_dev, own_dev), 1)
    earlier = jnp.where((row_i < col_i) & (t_col == t_row), 1.0, 0.0)
    position = jnp.sum(earlier, axis=0, keepdims=True)
    place = t_row * CAP + position
    which = lax.broadcasted_iota(jnp.int32, (devices * CAP, own_dev), 0).astype(jnp.float32)
    onehot = jnp.where(which == place, 1.0, 0.0).astype(jnp.bfloat16)
    outgoing = jnp.dot(onehot, owned_normed, preferred_element_type=jnp.float32).astype(jnp.bfloat16)
    dev_i = lax.broadcasted_iota(jnp.int32, (devices, own_dev), 0).astype(jnp.float32)
    lane_i = lax.broadcasted_iota(jnp.int32, (devices, LANES), 1)
    number = number_v[...].astype(jnp.float32) + 1.0
    outgoing_ids = jnp.full((devices, LANES), -1.0, jnp.float32)
    for k in range(CAP):
        here = jnp.where((dev_i == t_row) & (position == float(k)), number, 0.0)
        found = jnp.sum(here, axis=1, keepdims=True) - 1.0
        outgoing_ids = jnp.where(lane_i % CAP == k, found, outgoing_ids)
    outgoing_ids = outgoing_ids.astype(jnp.int32)
    for d in range(devices):
        obuf[d] = outgoing[d * CAP:(d + 1) * CAP, :]
        oid[d] = outgoing_ids[d:d + 1, :]

    keep_rows = pltpu.make_async_copy(obuf.at[me], rows_out.at[me], keep_sem.at[0])
    keep_ids = pltpu.make_async_copy(oid.at[me], ids_out.at[me], keep_sem.at[1])

    def start_routing():
        @pl.loop(1, devices)
        def _(step):
            other, og, ob = to_device(step)
            remote(obuf.at[other], rows_out.at[me], rows_send, rows_recv, ob, og).start()
            remote(oid.at[other], ids_out.at[me], oids_send, oids_recv, ob, og).start()

        keep_rows.start()
        keep_ids.start()

    def is_row(u, v):
        diff = (u - v + n_blk) % n_blk
        return (diff >= 1) & (diff <= CYCLE)

    slot_blocks = [b, partner, block_of(1), block_of(0), block_of(3)]

    def block_in(slot):
        result = slot_blocks[0]
        for i in range(1, 5):
            result = jnp.where(slot == i, slot_blocks[i], result)
        return result

    def run_units(table, phase, c):
        longest = max(len(entry) for by_phase in table for entry in by_phase)
        lists = [entry for by_phase in table for entry in by_phase]
        which_list = role * 2 + phase
        ends = [int(len(entry) > 0 and entry[-1] == OWN_PAIR) for entry in lists]
        count = pick(which_list, [len(entry) for entry in lists]) - pick(which_list, ends) * (1 - x)

        @pl.loop(0, count)
        def _(j):
            def entry(i):
                return pick(j * len(lists) + which_list,
                            [(lst[n] if n < len(lst) else (0, 0))[i] for n in range(longest) for lst in lists])

            u, v = entry(0), entry(1)
            bu, bv = block_in(u), block_in(v)

            @pl.when(is_row(bv, bu) | (u == v))
            def _():
                tile(v, whole, rows, u, span(c))

            @pl.when(is_row(bu, bv))
            def _():
                tile(u, span(c), ch, v, whole)

    def ids_wait(s):
        ids_copy(idv.at[s], 1, s, partner).wait_recv()

    def stream_wait(s, k):
        remote(raw.at[s, piece(k), :], raw.at[s, piece(k), :], send_sem.at[1, k], recv_sem.at[s, k], partner).wait_recv()

    routing_step = pick(role, [CHUNKS - 1, CHUNKS - 1, 2 * CHUNKS - 1, 2 * CHUNKS - 1])

    @pl.loop(0, 2 * CHUNKS)
    def _(p):
        phase = p // CHUNKS
        c = p % CHUNKS
        has_in = role > phase
        s_in = jnp.where((phase == 1) | (role == 1), ZERO, ONE)

        def take(k, first):
            @pl.when(has_in)
            def _():
                stream_wait(s_in, k)
                if first:
                    @pl.when(c == 0)
                    def _():
                        ids_wait(s_in)

                @pl.when(role < 3)
                def _():
                    onward_copy(s_in, k).start()
                    if first:
                        @pl.when(c == 0)
                        def _():
                            ids_copy(idv.at[s_in], s_in, s_in, onward).start()

            @pl.when((phase == 0) & (role == 3))
            def _():
                own_copy(k).start()

            @pl.when((phase == 0) & (role == 0))
            def _():
                own_copy(k).wait_send()

        take(2 * c, True)

        @pl.when((p == 2) & (role < 2) & gives_pair)
        def _():
            start_pair()

        run_units(UNITS_FIRST, phase, c)
        take(2 * c + 1, False)

        @pl.when(p == routing_step)
        def _():
            start_routing()

        @pl.when(has_in)
        def _():
            ready(s_in, c)

        @pl.when((early == (phase == 0)) & takes_pair)
        def _():
            @pl.when(c == 0)
            def _():
                ids_wait(PAIR)

            stream_wait(PAIR, 2 * c)
            stream_wait(PAIR, 2 * c + 1)
            ready(PAIR, c)

        @pl.when((role == 2) & (phase == 1))
        def _():
            @pl.when(c == 0)
            def _():
                ids_wait(THREE)

            stream_wait(THREE, 2 * c)
            stream_wait(THREE, 2 * c + 1)
            ready(THREE, c)

        run_units(UNITS_SECOND, phase, c)

    def back(slot, index, r):
        return remote(acc.at[slot], ret.at[index], ret_send.at[slot], ret_recv.at[index],
                      partner if r is None else block_of(r))

    returns = [(role > 0, PAIR, 0, None), (role == 1, ZERO, 1, 0), (role == 2, ZERO, 2, 0), (role == 3, ZERO, 3, 0),
               (role == 2, ONE, 2, 1), (role == 3, ONE, 3, 1), (role == 2, THREE, 2, 3)]
    for when, slot, index, r in reversed(returns):
        @pl.when(when)
        def _(slot=slot, index=index, r=r):
            back(slot, index, r).start()

    @pl.when(gives_pair)
    def _():
        ids_copy(ids, 1, PAIR, partner).wait_send()
        for k in range(pieces):
            pair_copy(k).wait_send()

    @pl.when(has_own)
    def _():
        ids_copy(ids, 0, own_slot, own_to).wait_send()

    @pl.when((role == 1) | (role == 3))
    def _():
        for k in range(pieces):
            own_copy(k).wait_send()

    for s, sends in ((ONE, role == 2), (ZERO, (role == 1) | (role == 2))):
        @pl.when(sends)
        def _(s=s):
            ids_copy(idv.at[s], s, s, onward).wait_send()
            for k in range(pieces):
                onward_copy(s, k).wait_send()

    keep_rows.wait()
    keep_ids.wait()
    others = pl.ds(0, devices - 1)
    pltpu.make_async_copy(obuf.at[others], rows_out.at[others], rows_send).wait()
    pltpu.make_async_copy(oid.at[others], ids_out.at[others], oids_send).wait()
    pltpu.make_async_copy(obuf.at[others], rows_out.at[others], rows_recv).wait()
    pltpu.make_async_copy(oid.at[others], ids_out.at[others], oids_recv).wait()

    run_out[...] = acc[OWN]
    for index, gets in enumerate((role > 0, role == 0, (role != 2), role < 2)):
        @pl.when(gets)
        def _(index=index):
            remote(acc.at[PAIR], ret.at[index], ret_send.at[PAIR], ret_recv.at[index], partner).wait_recv()
            run_out[...] = jnp.maximum(run_out[...], ret[index])

    for when, slot, index, r in returns:
        @pl.when(when)
        def _(slot=slot, index=index, r=r):
            back(slot, index, r).wait_send()


def place_kernel(run, routed, routed_ids, run_out, rows_out, ids_out):
    run_out[...] = run[...]
    devices, cap, _ = routed.shape
    for d in range(0, devices, 2):
        both = jnp.concatenate([routed[d].astype(jnp.float32), routed[d + 1].astype(jnp.float32)], axis=0)
        rows_out[d * cap:(d + 2) * cap, :] = both.astype(jnp.bfloat16)
    lines = routed_ids[...].reshape(devices, LANES)
    for part in range(devices * cap // LANES):
        sub = lines[part * LANES // cap:(part + 1) * LANES // cap, :]
        row_i = lax.broadcasted_iota(jnp.int32, sub.shape, 0)
        lane_i = lax.broadcasted_iota(jnp.int32, sub.shape, 1)
        mine = jnp.where(lane_i // cap == row_i, sub, 0)
        ids_out[:, part * LANES:(part + 1) * LANES] = jnp.sum(mine, axis=0, keepdims=True)


def body(embeds, doc_ids, prior_max, owned, owned_ids, owner_dest):
    n_grp, n_blk = lax.axis_size("grp"), lax.axis_size("blk")
    devices = n_grp * n_blk
    line = n_blk == 8
    rows, width = embeds.shape[1:]
    own_dev = owned.shape[0]
    vmem = pl.BlockSpec(memory_space=pltpu.VMEM)
    anywhere = pl.BlockSpec(memory_space=pl.ANY)
    dma = pltpu.SemaphoreType.DMA
    shapes = (
        jax.ShapeDtypeStruct((1, rows), jnp.float32),
        jax.ShapeDtypeStruct((devices, CAP, width), jnp.bfloat16),
        jax.ShapeDtypeStruct((devices, 1, LANES), jnp.int32),
    )
    limit = 60 * 1024 * 1024
    if line:
        slots, pieces = 5, 2 * CHUNKS
        results = pl.pallas_call(
            functools.partial(line_kernel, (n_grp, n_blk)),
            out_shape=shapes,
            in_specs=[anywhere] * 6,
            out_specs=(vmem, anywhere, anywhere),
            scratch_shapes=[
                pltpu.VMEM((slots, rows, width), jnp.bfloat16),
                pltpu.VMEM((slots, rows, width), jnp.bfloat16),
                pltpu.VMEM((slots, 1, rows), jnp.int32),
                pltpu.VMEM((slots, rows, LANES), jnp.float32),
                pltpu.VMEM((slots, 1, rows), jnp.float32),
                pltpu.VMEM((4, 1, rows), jnp.float32),
                pltpu.VMEM((devices, CAP, width), jnp.bfloat16),
                pltpu.VMEM((devices, 1, LANES), jnp.int32),
                pltpu.VMEM((1, rows), jnp.float32),
                pltpu.VMEM((own_dev, width), jnp.bfloat16),
                pltpu.VMEM((1, own_dev), jnp.int32),
                pltpu.VMEM((own_dev, 1, 1), jnp.int32),
                dma, dma((5,)), dma((slots, pieces)), dma((slots, pieces)),
                dma((slots,)), dma((slots,)), dma((slots,)), dma((4,)),
                dma, dma, dma, dma, dma((2,)),
            ],
            compiler_params=pltpu.CompilerParams(has_side_effects=True, collective_id=0, vmem_limit_bytes=limit),
        )(embeds, doc_ids, prior_max, owned, owned_ids.reshape(1, own_dev), owner_dest.reshape(own_dev, 1, 1))
    else:
        plan = make_plan(n_blk // 2)
        received, returns = plan[0], plan[5]
        slots = max(len(entry) for entry in received)
        results = pl.pallas_call(
            functools.partial(ring_kernel, plan, (n_grp, n_blk)),
            out_shape=shapes,
            in_specs=[anywhere, vmem, vmem, vmem, vmem, vmem],
            out_specs=(vmem, anywhere, anywhere),
            scratch_shapes=[
                pltpu.VMEM((2 + slots, rows, width), jnp.bfloat16),
                pltpu.VMEM((2 + slots, rows, width), jnp.bfloat16),
                pltpu.VMEM((2 + slots, 1, rows), jnp.int32),
                pltpu.VMEM((2 + slots, rows, LANES), jnp.float32),
                pltpu.VMEM((2 + slots, 1, rows), jnp.float32),
                pltpu.VMEM((1 + max(returns), 1, rows), jnp.float32),
                pltpu.VMEM((devices, CAP, width), jnp.bfloat16),
                pltpu.VMEM((devices, 1, LANES), jnp.int32),
                dma, dma((2 + slots, CHUNKS)), dma((2 + slots, CHUNKS)),
                dma((2 + slots,)), dma((2 + slots,)),
                dma((1 + slots,)), dma((1 + max(returns),)),
                dma, dma, dma, dma, dma((2,)),
            ],
            compiler_params=pltpu.CompilerParams(has_side_effects=True, vmem_limit_bytes=limit),
        )(embeds, doc_ids, prior_max, owned, owned_ids.reshape(1, own_dev), owner_dest)
    running, next_rows, next_ids = pl.pallas_call(
        place_kernel,
        out_shape=(
            jax.ShapeDtypeStruct((1, rows), jnp.float32),
            jax.ShapeDtypeStruct((devices * CAP, width), jnp.bfloat16),
            jax.ShapeDtypeStruct((1, devices * CAP), jnp.int32),
        ),
        in_specs=[vmem] * 3,
        out_specs=(vmem,) * 3,
    )(*results)
    return (running, next_rows, next_ids.reshape(devices * CAP))


def solution(mesh):
    return jax.shard_map(
        body,
        mesh=mesh,
        in_specs=(
            P("grp", "blk", None),
            P("grp", "blk"),
            P("grp", "blk"),
            P(("grp", "blk"), None),
            P(("grp", "blk")),
            P(("grp", "blk"), None),
        ),
        out_specs=(P("grp", "blk"), P(("grp", "blk"), None), P(("grp", "blk"))),
        check_vma=False,
    )
```

```python
import functools

import jax
import jax.numpy as jnp
from jax import lax
from jax.experimental import pallas as pl
from jax.experimental.pallas import tpu as pltpu
from jax.sharding import PartitionSpec as P

CYCLE = 3
CAP = 4
CHUNKS = 4
LANES = 128
EMPTY = -2.0


def make_plan(nz):
    received = [[((z - 1) % nz, (z - 1) % nz), ((z - 2) % nz, (z - 1) % nz)] for z in range(nz)]
    late = [False] * nz
    own_to = [(-1, 0)] * nz
    forward = [[(-1, 0)] * len(received[z]) for z in range(nz)]
    rank = [[0] * len(received[z]) for z in range(nz)]
    returns = [0] * nz
    for z in range(nz):
        for slot, (block, source) in enumerate(received[z]):
            if block == source:
                own_to[source] = (z, slot)
            else:
                held = [entry[0] for entry in received[source]].index(block)
                forward[source][held] = (z, slot)
            rank[z][slot] = returns[block]
            returns[block] += 1
    return received, own_to, late, forward, rank, returns


def pick(index, values):
    result = jnp.int32(values[0])
    for i in range(1, len(values)):
        if values[i] != values[0]:
            result = jnp.where(index == i, jnp.int32(values[i]), result)
    return result


def ring_kernel(plan, sizes, emb, ids, prior, owned, owned_ids, dest,
           run_out, rows_out, ids_out,
           raw, nrm, idv, idt, acc, ret, obuf, oid,
           local_sem, send_sem, recv_sem, ids_send, ids_recv, ret_send, ret_recv,
           rows_send, rows_recv, oids_send, oids_recv, keep_sem):
    n_grp, n_blk = sizes
    devices = n_grp * n_blk
    nz = n_blk // 2
    received, own_to, late, forward, rank, returns = plan
    slots = max(len(entry) for entry in received)
    rows = emb.shape[1]
    ch = rows // CHUNKS
    g = lax.axis_index("grp")
    b = lax.axis_index("blk")
    flip = g % 2
    z = b // 2
    x = b % 2
    role = z + flip * (nz - 1 - 2 * z)

    def block_of(zr):
        return 2 * (zr + flip * (nz - 1 - 2 * zr)) + x

    partner = b + 1 - 2 * x

    def table(values, slot=None, empty=0):
        if slot is None:
            return pick(role, values)
        return pick(role, [v[slot] if slot < len(v) else empty for v in values])

    own_z, own_slot = table([v[0] for v in own_to]), table([v[1] for v in own_to])
    is_late = table([int(v) for v in late])
    exists = [table([[1] * len(v) for v in received], s) for s in range(slots)]
    slot_z = [table([[e[0] for e in v] for v in received], s) for s in range(slots)]
    fwd_z = [table([[e[0] for e in v] for v in forward], s, -1) for s in range(slots)]
    fwd_slot = [table([[e[1] for e in v] for v in forward], s) for s in range(slots)]
    ranks = [table(rank, s) for s in range(slots)]
    n_returns = table(returns)
    blocks = [b, partner] + [block_of(slot_z[s]) for s in range(slots)]

    def span(c):
        if isinstance(c, int):
            return pl.ds(c * ch, ch)
        return pl.ds(pl.multiple_of(c * ch, ch), ch)

    def remote(src, dst, ssem, rsem, blk, grp=None):
        return pltpu.make_async_remote_copy(
            src_ref=src, dst_ref=dst, send_sem=ssem, recv_sem=rsem,
            device_id=(g if grp is None else grp, blk), device_id_type=pl.DeviceIdType.MESH)

    def chunk_copy(src, lane, to_slot, blk, c):
        return remote(src, raw.at[to_slot, span(c), :], send_sem.at[lane, c], recv_sem.at[to_slot, c], blk)

    def ids_copy(src, lane, to_slot, blk):
        return remote(src, idv.at[to_slot], ids_send.at[lane], ids_recv.at[to_slot], blk)

    def own_column(c):
        return chunk_copy(emb.at[0, span(c), :], 1, 2 + own_slot, block_of(own_z), c)

    def partner_copy(c):
        return chunk_copy(emb.at[0, span(c), :], 0, 1, partner, c)

    def forward_copy(s, c):
        return chunk_copy(raw.at[2 + s, span(c), :], 2 + s, 2 + fwd_slot[s], block_of(fwd_z[s]), c)

    def start_own_column():
        ids_copy(ids, 1, 2 + own_slot, block_of(own_z)).start()
        for c in range(CHUNKS):
            own_column(c).start()

    local = pltpu.make_async_copy(emb.at[0], raw.at[0], local_sem)
    local.start()

    @pl.when((own_z >= 0) & (is_late == 0))
    def _():
        start_own_column()

    ids_copy(ids, 0, 1, partner).start()
    for c in range(CHUNKS):
        partner_copy(c).start()

    def normalize(values):
        values = values.astype(jnp.float32)
        scale = lax.rsqrt(jnp.sum(values * values, axis=-1, keepdims=True) + 1e-06)
        return (values * scale).astype(jnp.bfloat16)

    own_dev = owned.shape[0]
    owned_normed = normalize(owned[...])
    t_col = dest[...].astype(jnp.float32)
    t_row = jnp.transpose(jnp.broadcast_to(t_col, (own_dev, LANES)))[0:1, :]
    row_i = lax.broadcasted_iota(jnp.int32, (own_dev, own_dev), 0)
    col_i = lax.broadcasted_iota(jnp.int32, (own_dev, own_dev), 1)
    earlier = jnp.where((row_i < col_i) & (t_col == t_row), 1.0, 0.0)
    position = jnp.sum(earlier, axis=0, keepdims=True)
    place = t_row * CAP + position
    which = lax.broadcasted_iota(jnp.int32, (devices * CAP, own_dev), 0).astype(jnp.float32)
    onehot = jnp.where(which == place, 1.0, 0.0).astype(jnp.bfloat16)
    outgoing = jnp.dot(onehot, owned_normed, preferred_element_type=jnp.float32).astype(jnp.bfloat16)
    dev_i = lax.broadcasted_iota(jnp.int32, (devices, own_dev), 0).astype(jnp.float32)
    lane_i = lax.broadcasted_iota(jnp.int32, (devices, LANES), 1)
    number = owned_ids[...].astype(jnp.float32) + 1.0
    outgoing_ids = jnp.full((devices, LANES), -1.0, jnp.float32)
    for k in range(CAP):
        here = jnp.where((dev_i == t_row) & (position == float(k)), number, 0.0)
        found = jnp.sum(here, axis=1, keepdims=True) - 1.0
        outgoing_ids = jnp.where(lane_i % CAP == k, found, outgoing_ids)
    outgoing_ids = outgoing_ids.astype(jnp.int32)
    for d in range(devices):
        obuf[d] = outgoing[d * CAP:(d + 1) * CAP, :]
        oid[d] = outgoing_ids[d:d + 1, :]

    def ready(s, c):
        at = span(c)
        nrm[s, at, :] = normalize(raw[s, at, :])
        for p in range(ch // LANES):
            at = pl.ds(pl.multiple_of(c * ch + p * LANES, LANES), LANES)
            line = idv[s, :, at].astype(jnp.float32)
            idt[s, at, :] = jnp.transpose(jnp.broadcast_to(line, (LANES, LANES)))

    def tile(row, row_at, width, col, col_at):
        scores = lax.dot_general(
            nrm[col, col_at, :], nrm[row, row_at, :], (((1,), (1,)), ((), ())),
            preferred_element_type=jnp.float32)
        row_ids = idv[row, :, row_at].astype(jnp.float32)
        col_ids = idt[col, col_at, :]
        parts = []
        for p in range(width // LANES):
            cut = slice(p * LANES, (p + 1) * LANES)
            masked = jnp.where(col_ids < row_ids[:, cut], scores[:, cut], EMPTY)
            parts.append(jnp.max(masked, axis=0, keepdims=True))
        acc[row, :, row_at] = jnp.maximum(acc[row, :, row_at], jnp.concatenate(parts, axis=1))

    whole = pl.ds(0, rows)

    acc[0] = prior[...]
    for s in range(1, 2 + slots):
        acc[s] = jnp.full((1, rows), EMPTY, jnp.float32)
    idv[0] = ids[...]
    local.wait()

    @pl.loop(0, CHUNKS)
    def _(c):
        ready(0, c)

    me = g * n_blk + b

    def to_device(step):
        other = (me + step) % devices
        return other, other // n_blk, other % n_blk

    @pl.loop(1, devices)
    def _(step):
        other, og, ob = to_device(step)
        remote(obuf.at[other], rows_out.at[me], rows_send, rows_recv, ob, og).start()
        remote(oid.at[other], ids_out.at[me], oids_send, oids_recv, ob, og).start()

    keep_rows = pltpu.make_async_copy(obuf.at[me], rows_out.at[me], keep_sem.at[0])
    keep_ids = pltpu.make_async_copy(oid.at[me], ids_out.at[me], keep_sem.at[1])
    keep_rows.start()
    keep_ids.start()

    def is_row(u, v):
        diff = (u - v + n_blk) % n_blk
        return (diff >= 1) & (diff <= CYCLE)

    def against_whole(s, c, other):
        @pl.when(is_row(blocks[s], blocks[other]))
        def _():
            tile(s, span(c), ch, other, whole)

        @pl.when(is_row(blocks[other], blocks[s]))
        def _():
            tile(other, whole, rows, s, span(c))

    def against_part(s, c, other, count):
        @pl.when(is_row(blocks[s], blocks[other]))
        def _():
            @pl.loop(0, count)
            def _(j):
                tile(s, span(c), ch, other, span(j))

        @pl.when(is_row(blocks[other], blocks[s]))
        def _():
            @pl.loop(0, count)
            def _(j):
                tile(other, span(j), ch, s, span(c))

    def arrive(s, c):
        chunk_copy(raw.at[s, span(c), :], 0, s, partner, c).wait_recv()

        @pl.when(c == 0)
        def _():
            ids_copy(idv.at[s], 0, s, partner).wait_recv()

        if s >= 2:
            @pl.when(fwd_z[s - 2] >= 0)
            def _():
                forward_copy(s - 2, c).start()

                @pl.when(c == 0)
                def _():
                    ids_copy(idv.at[s], s, 2 + fwd_slot[s - 2], block_of(fwd_z[s - 2])).start()

    @pl.loop(0, CHUNKS)
    def _(c):
        tile(0, whole, rows, 0, span(c))

    @pl.loop(0, CHUNKS)
    def _(c):
        @pl.when(exists[0] == 1)
        def _():
            arrive(2, c)
            ready(2, c)
            against_whole(2, c, 0)

    @pl.when((own_z >= 0) & (is_late == 1))
    def _():
        start_own_column()

    @pl.loop(0, CHUNKS)
    def _(c):
        for s in range(1, slots):
            @pl.when(exists[s] == 1)
            def _(s=s):
                arrive(2 + s, c)
                ready(2 + s, c)
                against_whole(2 + s, c, 0)
                against_part(2 + s, c, 1, c)

        arrive(1, c)
        ready(1, c)

        @pl.when(is_row(b, partner))
        def _():
            tile(0, whole, rows, 1, span(c))

        @pl.when(exists[0] == 1)
        def _():
            against_whole(1, c, 2)

        for s in range(1, slots):
            @pl.when(exists[s] == 1)
            def _(s=s):
                against_part(1, c, 2 + s, c + 1)

    back = remote(acc.at[1], ret.at[0], ret_send.at[0], ret_recv.at[0], partner)
    back.start()
    for s in range(slots):
        @pl.when(exists[s] == 1)
        def _(s=s):
            remote(acc.at[2 + s], ret.at[1 + ranks[s]], ret_send.at[1 + s], ret_recv.at[1 + ranks[s]],
                   block_of(slot_z[s])).start()

    for c in range(CHUNKS):
        partner_copy(c).wait_send()
    ids_copy(ids, 0, 1, partner).wait_send()

    @pl.when(own_z >= 0)
    def _():
        for c in range(CHUNKS):
            own_column(c).wait_send()
        ids_copy(ids, 1, 2 + own_slot, block_of(own_z)).wait_send()

    for s in range(slots):
        @pl.when(fwd_z[s] >= 0)
        def _(s=s):
            for c in range(CHUNKS):
                forward_copy(s, c).wait_send()
            ids_copy(idv.at[2 + s], 2 + s, 2 + fwd_slot[s], block_of(fwd_z[s])).wait_send()

    keep_rows.wait()
    keep_ids.wait()
    others = pl.ds(0, devices - 1)
    pltpu.make_async_copy(obuf.at[others], rows_out.at[others], rows_send).wait()
    pltpu.make_async_copy(oid.at[others], ids_out.at[others], oids_send).wait()
    pltpu.make_async_copy(obuf.at[others], rows_out.at[others], rows_recv).wait()
    pltpu.make_async_copy(oid.at[others], ids_out.at[others], oids_recv).wait()

    back.wait_recv()
    run_out[...] = jnp.maximum(acc[0], ret[0])
    for k in range(max(returns)):
        @pl.when(k < n_returns)
        def _(k=k):
            remote(acc.at[1], ret.at[1 + k], ret_send.at[0], ret_recv.at[1 + k], partner).wait_recv()
            run_out[...] = jnp.maximum(run_out[...], ret[1 + k])

    back.wait_send()
    for s in range(slots):
        @pl.when(exists[s] == 1)
        def _(s=s):
            remote(acc.at[2 + s], ret.at[1 + ranks[s]], ret_send.at[1 + s], ret_recv.at[1 + ranks[s]],
                   block_of(slot_z[s])).wait_send()


SPLIT = 4
LEAD = 4
LATE_LEAD = 4
LATE_STEP = 3
OWN, PAIR, ONE, ZERO, THREE = range(5)
SELF_UNIT = (OWN, OWN)
OWN_PAIR = (PAIR, OWN)
UNITS_FIRST = (
    ((SELF_UNIT,), ()),
    ((SELF_UNIT,), ()),
    ((SELF_UNIT,), ((ONE, PAIR), OWN_PAIR)),
    ((SELF_UNIT,), ((ONE, PAIR), OWN_PAIR)),
)
UNITS_SECOND = (
    ((), (OWN_PAIR,)),
    (((ZERO, OWN),), ((PAIR, ZERO), OWN_PAIR)),
    (((ONE, OWN),), ((ZERO, PAIR), (THREE, OWN), (THREE, PAIR))),
    ((), ((ZERO, OWN), (ZERO, PAIR))),
)


def line_kernel(sizes, emb, ids, prior, owned, owned_ids, dest,
                run_out, rows_out, ids_out,
                raw, nrm, idv, idt, acc, ret, obuf, oid, prior_v, owned_v, number_v, dest_v,
                local_sem, in_sem, send_sem, recv_sem, ids_send, ids_recv, ret_send, ret_recv,
                rows_send, rows_recv, oids_send, oids_recv, keep_sem, known_sem):
    n_grp, n_blk = sizes
    devices = n_grp * n_blk
    rows = emb.shape[1]
    ch = rows // CHUNKS
    part = ch // SPLIT
    g = lax.axis_index("grp")
    b = lax.axis_index("blk")
    flip = g % 2
    z = b // 2
    x = b % 2
    role = z + flip * (3 - 2 * z)
    partner = b + 1 - 2 * x
    me = g * n_blk + b

    def block_of(r):
        return 2 * (r + flip * (3 - 2 * r)) + x

    def to_device(step):
        other = (me + step) % devices
        return other, other // n_blk, other % n_blk

    barrier = pltpu.get_barrier_semaphore()

    def signal(semaphore, grp, blk):
        pl.semaphore_signal(semaphore, inc=1, device_id=(grp, blk), device_id_type=pl.DeviceIdType.MESH)

    other_core = g + 1 - 2 * flip
    other_row = (g + n_grp // 2) % n_grp
    signal(barrier, g, partner)
    signal(barrier, other_core, b)
    signal(barrier, other_row, b)

    @pl.when(z > 0)
    def _():
        signal(barrier, g, b - 2)

    @pl.when(z < 3)
    def _():
        signal(barrier, g, b + 2)

    local = pltpu.make_async_copy(emb.at[0], raw.at[OWN], local_sem)
    local.start()
    inputs = [pltpu.make_async_copy(src, dst, in_sem.at[i]) for i, (src, dst) in enumerate((
        (ids, idv.at[OWN]), (prior, prior_v), (owned, owned_v), (owned_ids, number_v), (dest, dest_v)))]
    for copy in inputs:
        copy.start()

    pl.semaphore_wait(barrier, jnp.where((z == 1) | (z == 2), 5, 4))

    def told(here, index, then=None):
        @pl.when(here)
        def _():
            if index is not None:
                pl.semaphore_wait(known_sem.at[index], 1)
            if then is not None:
                signal(known_sem.at[then[0]], then[1], then[2])

    told(z == 0, None, (0, g, b + 2))
    told(z == 3, None, (1, g, b - 2))

    def remote(src, dst, ssem, rsem, blk, grp=None):
        return pltpu.make_async_remote_copy(
            src_ref=src, dst_ref=dst, send_sem=ssem, recv_sem=rsem,
            device_id=(g if grp is None else grp, blk), device_id_type=pl.DeviceIdType.MESH)

    def piece(k):
        if isinstance(k, int):
            return pl.ds(k * part, part)
        return pl.ds(pl.multiple_of(k * part, part), part)

    def span(c):
        return pl.ds(pl.multiple_of(c * ch, ch), ch)

    whole = pl.ds(0, rows)
    pieces = SPLIT * CHUNKS

    own_slot = pick(role, [ZERO, ONE, ONE, THREE])
    own_to = block_of(pick(role, [1, 2, 3, 2]))
    has_own = role != 2
    onward = block_of(role + 1)
    gives_pair = (role > 0) | (x == 0)
    takes_pair = (role > 0) | (x == 1)
    early = role >= 2

    def own_copy(k):
        return remote(emb.at[0, piece(k), :], raw.at[own_slot, piece(k), :],
                      send_sem.at[0, k], recv_sem.at[own_slot, k], own_to)

    def pair_copy(k):
        return remote(emb.at[0, piece(k), :], raw.at[PAIR, piece(k), :],
                      send_sem.at[1, k], recv_sem.at[PAIR, k], partner)

    def onward_copy(s, k):
        return remote(raw.at[s, piece(k), :], raw.at[s, piece(k), :],
                      send_sem.at[s, k], recv_sem.at[s, k], onward)

    def ids_copy(src, lane, slot, blk):
        return remote(src, idv.at[slot], ids_send.at[lane], ids_recv.at[slot], blk)

    @pl.when(has_own)
    def _():
        ids_copy(ids, 0, own_slot, own_to).start()

    @pl.when(role < 2)
    def _():
        for k in range(pieces):
            own_copy(k).start()

    @pl.when(gives_pair)
    def _():
        ids_copy(ids, 1, PAIR, partner).start()

    @pl.when(early)
    def _():
        for k in range(LEAD):
            pair_copy(k).start()

    def normalize(values):
        values = values.astype(jnp.float32)
        scale = lax.rsqrt(jnp.sum(values * values, axis=-1, keepdims=True) + 1e-06)
        return (values * scale).astype(jnp.bfloat16)

    def ready(s, c):
        at = span(c)
        nrm[s, at, :] = normalize(raw[s, at, :])
        for p in range(ch // LANES):
            at = pl.ds(pl.multiple_of(c * ch + p * LANES, LANES), LANES)
            line = idv[s, :, at].astype(jnp.float32)
            idt[s, at, :] = jnp.transpose(jnp.broadcast_to(line, (LANES, LANES)))

    def tile(row, row_at, width, col, col_at):
        scores = lax.dot_general(
            nrm[col, col_at, :], nrm[row, row_at, :], (((1,), (1,)), ((), ())),
            preferred_element_type=jnp.float32)
        row_ids = idv[row, :, row_at].astype(jnp.float32)
        col_ids = idt[col, col_at, :]
        parts = []
        for p in range(width // LANES):
            cut = slice(p * LANES, (p + 1) * LANES)
            masked = jnp.where(col_ids < row_ids[:, cut], scores[:, cut], EMPTY)
            parts.append(jnp.max(masked, axis=0, keepdims=True))
        acc[row, :, row_at] = jnp.maximum(acc[row, :, row_at], jnp.concatenate(parts, axis=1))

    for s in range(1, 5):
        acc[s] = jnp.full((1, rows), EMPTY, jnp.float32)
    for copy in inputs:
        copy.wait()
    acc[OWN] = prior_v[...]
    local.wait()

    @pl.loop(0, CHUNKS)
    def _(c):
        ready(OWN, c)

    told(z == 1, 0, (0, g, b + 2))
    told(z == 2, 1, (1, g, b - 2))

    own_dev = owned.shape[0]
    owned_normed = normalize(owned_v[...])
    t_row = dest_v[...].astype(jnp.float32)
    t_col = jnp.transpose(jnp.broadcast_to(t_row, (LANES, own_dev)))[:, 0:1]
    row_i = lax.broadcasted_iota(jnp.int32, (own_dev, own_dev), 0)
    col_i = lax.broadcasted_iota(jnp.int32, (own_dev, own_dev), 1)
    earlier = jnp.where((row_i < col_i) & (t_col == t_row), 1.0, 0.0)
    position = jnp.sum(earlier, axis=0, keepdims=True)
    place = t_row * CAP + position
    which = lax.broadcasted_iota(jnp.int32, (devices * CAP, own_dev), 0).astype(jnp.float32)
    onehot = jnp.where(which == place, 1.0, 0.0).astype(jnp.bfloat16)
    outgoing = jnp.dot(onehot, owned_normed, preferred_element_type=jnp.float32).astype(jnp.bfloat16)
    dev_i = lax.broadcasted_iota(jnp.int32, (devices, own_dev), 0).astype(jnp.float32)
    lane_i = lax.broadcasted_iota(jnp.int32, (devices, LANES), 1)
    number = number_v[...].astype(jnp.float32) + 1.0
    outgoing_ids = jnp.full((devices, LANES), -1.0, jnp.float32)
    for k in range(CAP):
        here = jnp.where((dev_i == t_row) & (position == float(k)), number, 0.0)
        found = jnp.sum(here, axis=1, keepdims=True) - 1.0
        outgoing_ids = jnp.where(lane_i % CAP == k, found, outgoing_ids)
    outgoing_ids = outgoing_ids.astype(jnp.int32)
    for d in range(devices):
        obuf[d] = outgoing[d * CAP:(d + 1) * CAP, :]
        oid[d] = outgoing_ids[d:d + 1, :]

    told(z == 2, 0, (0, g, b + 2))
    told(z == 1, 1, (1, g, b - 2))

    keep_rows = pltpu.make_async_copy(obuf.at[me], rows_out.at[me], keep_sem.at[0])
    keep_ids = pltpu.make_async_copy(oid.at[me], ids_out.at[me], keep_sem.at[1])

    def start_routing():
        @pl.loop(1, devices)
        def _(step):
            other, og, ob = to_device(step)
            remote(obuf.at[other], rows_out.at[me], rows_send, rows_recv, ob, og).start()
            remote(oid.at[other], ids_out.at[me], oids_send, oids_recv, ob, og).start()

        keep_rows.start()
        keep_ids.start()

    def is_row(u, v):
        diff = (u - v + n_blk) % n_blk
        return (diff >= 1) & (diff <= CYCLE)

    slot_blocks = [b, partner, block_of(1), block_of(0), block_of(3)]

    def block_in(slot):
        result = slot_blocks[0]
        for i in range(1, 5):
            result = jnp.where(slot == i, slot_blocks[i], result)
        return result

    def run_units(table, phase, c):
        longest = max(len(entry) for by_phase in table for entry in by_phase)
        lists = [entry for by_phase in table for entry in by_phase]
        which_list = role * 2 + phase
        ends = [int(len(entry) > 0 and entry[-1] == OWN_PAIR) for entry in lists]
        count = pick(which_list, [len(entry) for entry in lists]) - pick(which_list, ends) * (1 - x)

        @pl.loop(0, count)
        def _(j):
            def entry(i):
                return pick(j * len(lists) + which_list,
                            [(lst[n] if n < len(lst) else (0, 0))[i] for n in range(longest) for lst in lists])

            u, v = entry(0), entry(1)
            bu, bv = block_in(u), block_in(v)

            @pl.when(is_row(bv, bu) | (u == v))
            def _():
                tile(v, whole, rows, u, span(c))

            @pl.when(is_row(bu, bv))
            def _():
                tile(u, span(c), ch, v, whole)

    def ids_wait(s):
        ids_copy(idv.at[s], 1, s, partner).wait_recv()

    def stream_wait(s, k):
        remote(raw.at[s, piece(k), :], raw.at[s, piece(k), :], send_sem.at[1, k], recv_sem.at[s, k], partner).wait_recv()

    @pl.loop(0, 2 * CHUNKS)
    def _(p):
        phase = p // CHUNKS
        c = p % CHUNKS
        has_in = role > phase
        s_in = jnp.where((phase == 1) | (role == 1), ZERO, ONE)

        def take(i):
            k = SPLIT * c + i

            @pl.when(has_in)
            def _():
                stream_wait(s_in, k)
                if i == 0:
                    @pl.when(c == 0)
                    def _():
                        ids_wait(s_in)

                @pl.when(role < 3)
                def _():
                    onward_copy(s_in, k).start()
                    if i == 0:
                        @pl.when(c == 0)
                        def _():
                            ids_copy(idv.at[s_in], s_in, s_in, onward).start()

            @pl.when((phase == 0) & (role == 0))
            def _():
                own_copy(k).wait_send()

            @pl.when((phase == 0) & early & (k + LEAD < pieces))
            def _():
                pair_copy(k + LEAD).start()

            @pl.when((phase == 0) & (role == 3) & (k >= pieces // 2))
            def _():
                own_copy(2 * k - pieces).start()
                own_copy(2 * k - pieces + 1).start()

            if i == 0:
                @pl.when((phase == 1) & (role < 2) & takes_pair & (c == 0))
                def _():
                    ids_wait(PAIR)

            @pl.when((phase == 1) & (role < 2) & takes_pair)
            def _():
                stream_wait(PAIR, k)

            @pl.when((phase == 1) & (role == 0) & gives_pair)
            def _():
                pair_copy(k).wait_send()

            @pl.when((phase == 1) & (role < 2) & gives_pair & (k + LATE_LEAD < pieces))
            def _():
                pair_copy(k + LATE_LEAD).start()

        for i in range(SPLIT // 2):
            take(i)

        @pl.when((p == LATE_STEP) & (role < 2) & gives_pair)
        def _():
            for k in range(LATE_LEAD):
                pair_copy(k).start()

        @pl.when((p == 2 * CHUNKS - 1) & (role != 2))
        def _():
            start_routing()

        run_units(UNITS_FIRST, phase, c)
        for i in range(SPLIT // 2, SPLIT):
            take(i)

        @pl.when((p == 2 * CHUNKS - 1) & (role == 2))
        def _():
            start_routing()

        told((p == 0) & (z == 3), 0)
        told((p == 0) & (z == 0), 1)
        told(p == 0, None, (2, other_core, b))
        told(p == 1, 2, (3, other_row, b))
        told(p == 2, 3)

        @pl.when(has_in)
        def _():
            ready(s_in, c)

        @pl.when((phase == 0) & early)
        def _():
            @pl.when(c == 0)
            def _():
                ids_wait(PAIR)

            for i in range(SPLIT):
                stream_wait(PAIR, SPLIT * c + i)

        @pl.when((early == (phase == 0)) & takes_pair)
        def _():
            ready(PAIR, c)

        @pl.when((role == 2) & (phase == 1))
        def _():
            @pl.when(c == 0)
            def _():
                ids_wait(THREE)

            for i in range(SPLIT):
                stream_wait(THREE, SPLIT * c + i)
            ready(THREE, c)

        run_units(UNITS_SECOND, phase, c)

    def back(slot, index, r):
        return remote(acc.at[slot], ret.at[index], ret_send.at[slot], ret_recv.at[index],
                      partner if r is None else block_of(r))

    returns = [(role > 0, PAIR, 0, None), (role == 1, ZERO, 1, 0), (role == 2, ZERO, 2, 0), (role == 3, ZERO, 3, 0),
               (role == 2, ONE, 2, 1), (role == 3, ONE, 3, 1), (role == 2, THREE, 2, 3)]
    for when, slot, index, r in reversed(returns):
        @pl.when(when)
        def _(slot=slot, index=index, r=r):
            back(slot, index, r).start()

    @pl.when(gives_pair)
    def _():
        ids_copy(ids, 1, PAIR, partner).wait_send()

    @pl.when(role > 0)
    def _():
        for k in range(pieces):
            pair_copy(k).wait_send()

    @pl.when(has_own)
    def _():
        ids_copy(ids, 0, own_slot, own_to).wait_send()

    @pl.when((role == 1) | (role == 3))
    def _():
        for k in range(pieces):
            own_copy(k).wait_send()

    for s, sends in ((ONE, role == 2), (ZERO, (role == 1) | (role == 2))):
        @pl.when(sends)
        def _(s=s):
            ids_copy(idv.at[s], s, s, onward).wait_send()
            for k in range(pieces):
                onward_copy(s, k).wait_send()

    keep_rows.wait()
    keep_ids.wait()
    others = pl.ds(0, devices - 1)
    pltpu.make_async_copy(obuf.at[others], rows_out.at[others], rows_send).wait()
    pltpu.make_async_copy(oid.at[others], ids_out.at[others], oids_send).wait()
    pltpu.make_async_copy(obuf.at[others], rows_out.at[others], rows_recv).wait()
    pltpu.make_async_copy(oid.at[others], ids_out.at[others], oids_recv).wait()

    run_out[...] = acc[OWN]
    for index, gets in enumerate((role > 0, role == 0, (role != 2), role < 2)):
        @pl.when(gets)
        def _(index=index):
            remote(acc.at[PAIR], ret.at[index], ret_send.at[PAIR], ret_recv.at[index], partner).wait_recv()
            run_out[...] = jnp.maximum(run_out[...], ret[index])

    for when, slot, index, r in returns:
        @pl.when(when)
        def _(slot=slot, index=index, r=r):
            back(slot, index, r).wait_send()


def place_kernel(run, routed, routed_ids, run_out, rows_out, ids_out):
    run_out[...] = run[...]
    devices, cap, _ = routed.shape
    for d in range(0, devices, 2):
        both = jnp.concatenate([routed[d].astype(jnp.float32), routed[d + 1].astype(jnp.float32)], axis=0)
        rows_out[d * cap:(d + 2) * cap, :] = both.astype(jnp.bfloat16)
    lines = routed_ids[...].reshape(devices, LANES)
    for part in range(devices * cap // LANES):
        sub = lines[part * LANES // cap:(part + 1) * LANES // cap, :]
        row_i = lax.broadcasted_iota(jnp.int32, sub.shape, 0)
        lane_i = lax.broadcasted_iota(jnp.int32, sub.shape, 1)
        mine = jnp.where(lane_i // cap == row_i, sub, 0)
        ids_out[:, part * LANES:(part + 1) * LANES] = jnp.sum(mine, axis=0, keepdims=True)


def body(embeds, doc_ids, prior_max, owned, owned_ids, owner_dest):
    n_grp, n_blk = lax.axis_size("grp"), lax.axis_size("blk")
    devices = n_grp * n_blk
    line = (n_grp, n_blk) == (4, 8)
    rows, width = embeds.shape[1:]
    own_dev = owned.shape[0]
    vmem = pl.BlockSpec(memory_space=pltpu.VMEM)
    anywhere = pl.BlockSpec(memory_space=pl.ANY)
    dma = pltpu.SemaphoreType.DMA
    shapes = (
        jax.ShapeDtypeStruct((1, rows), jnp.float32),
        jax.ShapeDtypeStruct((devices, CAP, width), jnp.bfloat16),
        jax.ShapeDtypeStruct((devices, 1, LANES), jnp.int32),
    )
    limit = 60 * 1024 * 1024
    if line:
        slots, pieces = 5, SPLIT * CHUNKS
        results = pl.pallas_call(
            functools.partial(line_kernel, (n_grp, n_blk)),
            out_shape=shapes,
            in_specs=[anywhere] * 6,
            out_specs=(vmem, anywhere, anywhere),
            scratch_shapes=[
                pltpu.VMEM((slots, rows, width), jnp.bfloat16),
                pltpu.VMEM((slots, rows, width), jnp.bfloat16),
                pltpu.VMEM((slots, 1, rows), jnp.int32),
                pltpu.VMEM((slots, rows, LANES), jnp.float32),
                pltpu.VMEM((slots, 1, rows), jnp.float32),
                pltpu.VMEM((4, 1, rows), jnp.float32),
                pltpu.VMEM((devices, CAP, width), jnp.bfloat16),
                pltpu.VMEM((devices, 1, LANES), jnp.int32),
                pltpu.VMEM((1, rows), jnp.float32),
                pltpu.VMEM((own_dev, width), jnp.bfloat16),
                pltpu.VMEM((1, own_dev), jnp.int32),
                pltpu.VMEM((1, own_dev), jnp.int32),
                dma, dma((5,)), dma((slots, pieces)), dma((slots, pieces)),
                dma((slots,)), dma((slots,)), dma((slots,)), dma((4,)),
                dma, dma, dma, dma, dma((2,)), pltpu.SemaphoreType.REGULAR((4,)),
            ],
            compiler_params=pltpu.CompilerParams(has_side_effects=True, collective_id=0, vmem_limit_bytes=limit),
        )(embeds, doc_ids, prior_max, owned, owned_ids.reshape(1, own_dev), owner_dest.reshape(1, own_dev))
    else:
        plan = make_plan(n_blk // 2)
        received, returns = plan[0], plan[5]
        slots = max(len(entry) for entry in received)
        results = pl.pallas_call(
            functools.partial(ring_kernel, plan, (n_grp, n_blk)),
            out_shape=shapes,
            in_specs=[anywhere, vmem, vmem, vmem, vmem, vmem],
            out_specs=(vmem, anywhere, anywhere),
            scratch_shapes=[
                pltpu.VMEM((2 + slots, rows, width), jnp.bfloat16),
                pltpu.VMEM((2 + slots, rows, width), jnp.bfloat16),
                pltpu.VMEM((2 + slots, 1, rows), jnp.int32),
                pltpu.VMEM((2 + slots, rows, LANES), jnp.float32),
                pltpu.VMEM((2 + slots, 1, rows), jnp.float32),
                pltpu.VMEM((1 + max(returns), 1, rows), jnp.float32),
                pltpu.VMEM((devices, CAP, width), jnp.bfloat16),
                pltpu.VMEM((devices, 1, LANES), jnp.int32),
                dma, dma((2 + slots, CHUNKS)), dma((2 + slots, CHUNKS)),
                dma((2 + slots,)), dma((2 + slots,)),
                dma((1 + slots,)), dma((1 + max(returns),)),
                dma, dma, dma, dma, dma((2,)),
            ],
            compiler_params=pltpu.CompilerParams(has_side_effects=True, vmem_limit_bytes=limit),
        )(embeds, doc_ids, prior_max, owned, owned_ids.reshape(1, own_dev), owner_dest)
    running, next_rows, next_ids = pl.pallas_call(
        place_kernel,
        out_shape=(
            jax.ShapeDtypeStruct((1, rows), jnp.float32),
            jax.ShapeDtypeStruct((devices * CAP, width), jnp.bfloat16),
            jax.ShapeDtypeStruct((1, devices * CAP), jnp.int32),
        ),
        in_specs=[vmem] * 3,
        out_specs=(vmem,) * 3,
    )(*results)
    return (running, next_rows, next_ids.reshape(devices * CAP))


def solution(mesh):
    return jax.shard_map(
        body,
        mesh=mesh,
        in_specs=(
            P("grp", "blk", None),
            P("grp", "blk"),
            P("grp", "blk"),
            P(("grp", "blk"), None),
            P(("grp", "blk")),
            P(("grp", "blk"), None),
        ),
        out_specs=(P("grp", "blk"), P(("grp", "blk"), None), P(("grp", "blk"))),
        check_vma=False,
    )
```

```python
import functools

import jax
import jax.numpy as jnp
from jax import lax
from jax.experimental import pallas as pl
from jax.experimental.pallas import tpu as pltpu
from jax.sharding import PartitionSpec as P

CYCLE = 3
CAP = 4
CHUNKS = 4
LANES = 128
EMPTY = -2.0


def make_plan(nz):
    received = [[((z - 1) % nz, (z - 1) % nz), ((z - 2) % nz, (z - 1) % nz)] for z in range(nz)]
    late = [False] * nz
    own_to = [(-1, 0)] * nz
    forward = [[(-1, 0)] * len(received[z]) for z in range(nz)]
    rank = [[0] * len(received[z]) for z in range(nz)]
    returns = [0] * nz
    for z in range(nz):
        for slot, (block, source) in enumerate(received[z]):
            if block == source:
                own_to[source] = (z, slot)
            else:
                held = [entry[0] for entry in received[source]].index(block)
                forward[source][held] = (z, slot)
            rank[z][slot] = returns[block]
            returns[block] += 1
    return received, own_to, late, forward, rank, returns


def pick(index, values):
    result = jnp.int32(values[0])
    for i in range(1, len(values)):
        if values[i] != values[0]:
            result = jnp.where(index == i, jnp.int32(values[i]), result)
    return result


def ring_kernel(plan, sizes, emb, ids, prior, owned, owned_ids, dest,
           run_out, rows_out, ids_out,
           raw, nrm, idv, idt, acc, ret, obuf, oid,
           local_sem, send_sem, recv_sem, ids_send, ids_recv, ret_send, ret_recv,
           rows_send, rows_recv, oids_send, oids_recv, keep_sem):
    n_grp, n_blk = sizes
    devices = n_grp * n_blk
    nz = n_blk // 2
    received, own_to, late, forward, rank, returns = plan
    slots = max(len(entry) for entry in received)
    rows = emb.shape[1]
    ch = rows // CHUNKS
    g = lax.axis_index("grp")
    b = lax.axis_index("blk")
    flip = g % 2
    z = b // 2
    x = b % 2
    role = z + flip * (nz - 1 - 2 * z)

    def block_of(zr):
        return 2 * (zr + flip * (nz - 1 - 2 * zr)) + x

    partner = b + 1 - 2 * x

    def table(values, slot=None, empty=0):
        if slot is None:
            return pick(role, values)
        return pick(role, [v[slot] if slot < len(v) else empty for v in values])

    own_z, own_slot = table([v[0] for v in own_to]), table([v[1] for v in own_to])
    is_late = table([int(v) for v in late])
    exists = [table([[1] * len(v) for v in received], s) for s in range(slots)]
    slot_z = [table([[e[0] for e in v] for v in received], s) for s in range(slots)]
    fwd_z = [table([[e[0] for e in v] for v in forward], s, -1) for s in range(slots)]
    fwd_slot = [table([[e[1] for e in v] for v in forward], s) for s in range(slots)]
    ranks = [table(rank, s) for s in range(slots)]
    n_returns = table(returns)
    blocks = [b, partner] + [block_of(slot_z[s]) for s in range(slots)]

    def span(c):
        if isinstance(c, int):
            return pl.ds(c * ch, ch)
        return pl.ds(pl.multiple_of(c * ch, ch), ch)

    def remote(src, dst, ssem, rsem, blk, grp=None):
        return pltpu.make_async_remote_copy(
            src_ref=src, dst_ref=dst, send_sem=ssem, recv_sem=rsem,
            device_id=(g if grp is None else grp, blk), device_id_type=pl.DeviceIdType.MESH)

    def chunk_copy(src, lane, to_slot, blk, c):
        return remote(src, raw.at[to_slot, span(c), :], send_sem.at[lane, c], recv_sem.at[to_slot, c], blk)

    def ids_copy(src, lane, to_slot, blk):
        return remote(src, idv.at[to_slot], ids_send.at[lane], ids_recv.at[to_slot], blk)

    def own_column(c):
        return chunk_copy(emb.at[0, span(c), :], 1, 2 + own_slot, block_of(own_z), c)

    def partner_copy(c):
        return chunk_copy(emb.at[0, span(c), :], 0, 1, partner, c)

    def forward_copy(s, c):
        return chunk_copy(raw.at[2 + s, span(c), :], 2 + s, 2 + fwd_slot[s], block_of(fwd_z[s]), c)

    def start_own_column():
        ids_copy(ids, 1, 2 + own_slot, block_of(own_z)).start()
        for c in range(CHUNKS):
            own_column(c).start()

    local = pltpu.make_async_copy(emb.at[0], raw.at[0], local_sem)
    local.start()

    @pl.when((own_z >= 0) & (is_late == 0))
    def _():
        start_own_column()

    ids_copy(ids, 0, 1, partner).start()
    for c in range(CHUNKS):
        partner_copy(c).start()

    def normalize(values):
        values = values.astype(jnp.float32)
        scale = lax.rsqrt(jnp.sum(values * values, axis=-1, keepdims=True) + 1e-06)
        return (values * scale).astype(jnp.bfloat16)

    own_dev = owned.shape[0]
    owned_normed = normalize(owned[...])
    t_col = dest[...].astype(jnp.float32)
    t_row = jnp.transpose(jnp.broadcast_to(t_col, (own_dev, LANES)))[0:1, :]
    row_i = lax.broadcasted_iota(jnp.int32, (own_dev, own_dev), 0)
    col_i = lax.broadcasted_iota(jnp.int32, (own_dev, own_dev), 1)
    earlier = jnp.where((row_i < col_i) & (t_col == t_row), 1.0, 0.0)
    position = jnp.sum(earlier, axis=0, keepdims=True)
    place = t_row * CAP + position
    which = lax.broadcasted_iota(jnp.int32, (devices * CAP, own_dev), 0).astype(jnp.float32)
    onehot = jnp.where(which == place, 1.0, 0.0).astype(jnp.bfloat16)
    outgoing = jnp.dot(onehot, owned_normed, preferred_element_type=jnp.float32).astype(jnp.bfloat16)
    dev_i = lax.broadcasted_iota(jnp.int32, (devices, own_dev), 0).astype(jnp.float32)
    lane_i = lax.broadcasted_iota(jnp.int32, (devices, LANES), 1)
    number = owned_ids[...].astype(jnp.float32) + 1.0
    outgoing_ids = jnp.full((devices, LANES), -1.0, jnp.float32)
    for k in range(CAP):
        here = jnp.where((dev_i == t_row) & (position == float(k)), number, 0.0)
        found = jnp.sum(here, axis=1, keepdims=True) - 1.0
        outgoing_ids = jnp.where(lane_i % CAP == k, found, outgoing_ids)
    outgoing_ids = outgoing_ids.astype(jnp.int32)
    for d in range(devices):
        obuf[d] = outgoing[d * CAP:(d + 1) * CAP, :]
        oid[d] = outgoing_ids[d:d + 1, :]

    def ready(s, c):
        at = span(c)
        nrm[s, at, :] = normalize(raw[s, at, :])
        for p in range(ch // LANES):
            at = pl.ds(pl.multiple_of(c * ch + p * LANES, LANES), LANES)
            line = idv[s, :, at].astype(jnp.float32)
            idt[s, at, :] = jnp.transpose(jnp.broadcast_to(line, (LANES, LANES)))

    def tile(row, row_at, width, col, col_at):
        scores = lax.dot_general(
            nrm[col, col_at, :], nrm[row, row_at, :], (((1,), (1,)), ((), ())),
            preferred_element_type=jnp.float32)
        row_ids = idv[row, :, row_at].astype(jnp.float32)
        col_ids = idt[col, col_at, :]
        parts = []
        for p in range(width // LANES):
            cut = slice(p * LANES, (p + 1) * LANES)
            masked = jnp.where(col_ids < row_ids[:, cut], scores[:, cut], EMPTY)
            parts.append(jnp.max(masked, axis=0, keepdims=True))
        acc[row, :, row_at] = jnp.maximum(acc[row, :, row_at], jnp.concatenate(parts, axis=1))

    whole = pl.ds(0, rows)

    acc[0] = prior[...]
    for s in range(1, 2 + slots):
        acc[s] = jnp.full((1, rows), EMPTY, jnp.float32)
    idv[0] = ids[...]
    local.wait()

    @pl.loop(0, CHUNKS)
    def _(c):
        ready(0, c)

    me = g * n_blk + b

    def to_device(step):
        other = (me + step) % devices
        return other, other // n_blk, other % n_blk

    @pl.loop(1, devices)
    def _(step):
        other, og, ob = to_device(step)
        remote(obuf.at[other], rows_out.at[me], rows_send, rows_recv, ob, og).start()
        remote(oid.at[other], ids_out.at[me], oids_send, oids_recv, ob, og).start()

    keep_rows = pltpu.make_async_copy(obuf.at[me], rows_out.at[me], keep_sem.at[0])
    keep_ids = pltpu.make_async_copy(oid.at[me], ids_out.at[me], keep_sem.at[1])
    keep_rows.start()
    keep_ids.start()

    def is_row(u, v):
        diff = (u - v + n_blk) % n_blk
        return (diff >= 1) & (diff <= CYCLE)

    def against_whole(s, c, other):
        @pl.when(is_row(blocks[s], blocks[other]))
        def _():
            tile(s, span(c), ch, other, whole)

        @pl.when(is_row(blocks[other], blocks[s]))
        def _():
            tile(other, whole, rows, s, span(c))

    def against_part(s, c, other, count):
        @pl.when(is_row(blocks[s], blocks[other]))
        def _():
            @pl.loop(0, count)
            def _(j):
                tile(s, span(c), ch, other, span(j))

        @pl.when(is_row(blocks[other], blocks[s]))
        def _():
            @pl.loop(0, count)
            def _(j):
                tile(other, span(j), ch, s, span(c))

    def arrive(s, c):
        chunk_copy(raw.at[s, span(c), :], 0, s, partner, c).wait_recv()

        @pl.when(c == 0)
        def _():
            ids_copy(idv.at[s], 0, s, partner).wait_recv()

        if s >= 2:
            @pl.when(fwd_z[s - 2] >= 0)
            def _():
                forward_copy(s - 2, c).start()

                @pl.when(c == 0)
                def _():
                    ids_copy(idv.at[s], s, 2 + fwd_slot[s - 2], block_of(fwd_z[s - 2])).start()

    @pl.loop(0, CHUNKS)
    def _(c):
        tile(0, whole, rows, 0, span(c))

    @pl.loop(0, CHUNKS)
    def _(c):
        @pl.when(exists[0] == 1)
        def _():
            arrive(2, c)
            ready(2, c)
            against_whole(2, c, 0)

    @pl.when((own_z >= 0) & (is_late == 1))
    def _():
        start_own_column()

    @pl.loop(0, CHUNKS)
    def _(c):
        for s in range(1, slots):
            @pl.when(exists[s] == 1)
            def _(s=s):
                arrive(2 + s, c)
                ready(2 + s, c)
                against_whole(2 + s, c, 0)
                against_part(2 + s, c, 1, c)

        arrive(1, c)
        ready(1, c)

        @pl.when(is_row(b, partner))
        def _():
            tile(0, whole, rows, 1, span(c))

        @pl.when(exists[0] == 1)
        def _():
            against_whole(1, c, 2)

        for s in range(1, slots):
            @pl.when(exists[s] == 1)
            def _(s=s):
                against_part(1, c, 2 + s, c + 1)

    back = remote(acc.at[1], ret.at[0], ret_send.at[0], ret_recv.at[0], partner)
    back.start()
    for s in range(slots):
        @pl.when(exists[s] == 1)
        def _(s=s):
            remote(acc.at[2 + s], ret.at[1 + ranks[s]], ret_send.at[1 + s], ret_recv.at[1 + ranks[s]],
                   block_of(slot_z[s])).start()

    for c in range(CHUNKS):
        partner_copy(c).wait_send()
    ids_copy(ids, 0, 1, partner).wait_send()

    @pl.when(own_z >= 0)
    def _():
        for c in range(CHUNKS):
            own_column(c).wait_send()
        ids_copy(ids, 1, 2 + own_slot, block_of(own_z)).wait_send()

    for s in range(slots):
        @pl.when(fwd_z[s] >= 0)
        def _(s=s):
            for c in range(CHUNKS):
                forward_copy(s, c).wait_send()
            ids_copy(idv.at[2 + s], 2 + s, 2 + fwd_slot[s], block_of(fwd_z[s])).wait_send()

    keep_rows.wait()
    keep_ids.wait()
    others = pl.ds(0, devices - 1)
    pltpu.make_async_copy(obuf.at[others], rows_out.at[others], rows_send).wait()
    pltpu.make_async_copy(oid.at[others], ids_out.at[others], oids_send).wait()
    pltpu.make_async_copy(obuf.at[others], rows_out.at[others], rows_recv).wait()
    pltpu.make_async_copy(oid.at[others], ids_out.at[others], oids_recv).wait()

    back.wait_recv()
    run_out[...] = jnp.maximum(acc[0], ret[0])
    for k in range(max(returns)):
        @pl.when(k < n_returns)
        def _(k=k):
            remote(acc.at[1], ret.at[1 + k], ret_send.at[0], ret_recv.at[1 + k], partner).wait_recv()
            run_out[...] = jnp.maximum(run_out[...], ret[1 + k])

    back.wait_send()
    for s in range(slots):
        @pl.when(exists[s] == 1)
        def _(s=s):
            remote(acc.at[2 + s], ret.at[1 + ranks[s]], ret_send.at[1 + s], ret_recv.at[1 + ranks[s]],
                   block_of(slot_z[s])).wait_send()


SPLIT = 4
LATE_LEAD = 2
LATE_STEP = 3
THREE_FROM = 7
OWN, PAIR, ONE, ZERO, THREE = range(5)
SELF_UNIT = (OWN, OWN)
OWN_PAIR = (PAIR, OWN)
UNITS = (
    (((), ()), ((), ()), ((), ((THREE, OWN),)), ((), ())),
    (((SELF_UNIT,), ()), ((SELF_UNIT,), ()), ((SELF_UNIT,), ((ZERO, PAIR),)), ((SELF_UNIT,), ((ZERO, PAIR),))),
    (((), ()), ((), ()), ((), ((THREE, PAIR),)), ((), ())),
    (((), (OWN_PAIR,)), (((ZERO, OWN),), ((PAIR, ZERO), OWN_PAIR)),
     ((OWN_PAIR,), ((ONE, OWN), (ONE, PAIR))), (((ZERO, OWN), OWN_PAIR), ((ONE, PAIR),))),
)


def line_kernel(sizes, emb, ids, prior, owned, owned_ids, dest,
                run_out, rows_out, ids_out, ret,
                raw, nrm, idv, idt, acc, obuf, oid, prior_v, owned_v, number_v, dest_v,
                local_sem, in_sem, send_sem, recv_sem, block_recv, ids_send, ids_recv, ret_send, ret_recv,
                rows_send, rows_recv, oids_send, oids_recv, keep_sem, known_sem):
    n_grp, n_blk = sizes
    devices = n_grp * n_blk
    rows = emb.shape[1]
    ch = rows // CHUNKS
    part = ch // SPLIT
    g = lax.axis_index("grp")
    b = lax.axis_index("blk")
    flip = g % 2
    z = b // 2
    x = b % 2
    role = z + flip * (3 - 2 * z)
    partner = b + 1 - 2 * x
    me = g * n_blk + b

    def block_of(r):
        return 2 * (r + flip * (3 - 2 * r)) + x

    def to_device(step):
        turn = (step - 1) // n_blk
        u = (step - 1) % n_blk + turn // (n_grp - 1)
        og = (g + u // 2) % n_grp
        oz = pick(4 * z + turn, [2, 1, 3, 0, 2, 3, 0, 1, 1, 0, 3, 2, 1, 2, 0, 3])
        ob = 2 * oz + (x + u) % 2
        return og * n_blk + ob, og, ob

    barrier = pltpu.get_barrier_semaphore()

    def signal(semaphore, grp, blk):
        pl.semaphore_signal(semaphore, inc=1, device_id=(grp, blk), device_id_type=pl.DeviceIdType.MESH)

    other_core = g + 1 - 2 * flip
    other_row = (g + n_grp // 2) % n_grp
    signal(barrier, g, partner)
    signal(barrier, other_core, b)
    signal(barrier, other_row, b)

    @pl.when(z > 0)
    def _():
        signal(barrier, g, b - 2)

    @pl.when(z < 3)
    def _():
        signal(barrier, g, b + 2)

    local = pltpu.make_async_copy(emb.at[0], raw.at[OWN], local_sem)
    local.start()
    inputs = [pltpu.make_async_copy(src, dst, in_sem.at[i]) for i, (src, dst) in enumerate((
        (ids, idv.at[OWN]), (prior, prior_v), (owned, owned_v), (owned_ids, number_v), (dest, dest_v)))]
    for copy in inputs:
        copy.start()

    pl.semaphore_wait(barrier, jnp.where((z == 1) | (z == 2), 5, 4))

    def told(here, index, then=None):
        @pl.when(here)
        def _():
            if index is not None:
                pl.semaphore_wait(known_sem.at[index], 1)
            if then is not None:
                signal(known_sem.at[then[0]], then[1], then[2])

    told(z == 0, None, (0, g, b + 2))
    told(z == 3, None, (1, g, b - 2))

    def remote(src, dst, ssem, rsem, blk, grp=None):
        return pltpu.make_async_remote_copy(
            src_ref=src, dst_ref=dst, send_sem=ssem, recv_sem=rsem,
            device_id=(g if grp is None else grp, blk), device_id_type=pl.DeviceIdType.MESH)

    def piece(k):
        if isinstance(k, int):
            return pl.ds(k * part, part)
        return pl.ds(pl.multiple_of(k * part, part), part)

    def span(c):
        if isinstance(c, int):
            return pl.ds(c * ch, ch)
        return pl.ds(pl.multiple_of(c * ch, ch), ch)

    whole = pl.ds(0, rows)
    pieces = SPLIT * CHUNKS

    own_slot = pick(role, [ZERO, ONE, ONE, THREE])
    own_to = block_of(pick(role, [1, 2, 3, 2]))
    has_own = role != 2
    onward = block_of(role + 1)
    gives_pair = (role > 0) | (x == 0)
    takes_pair = (role > 0) | (x == 1)
    early = role >= 2

    def own_copy(k, sem):
        return remote(emb.at[0, piece(k), :], raw.at[own_slot, piece(k), :],
                      send_sem.at[0, k // SPLIT], sem, own_to)

    def pair_copy(k):
        return remote(emb.at[0, piece(k), :], raw.at[PAIR, piece(k), :],
                      send_sem.at[1, k // SPLIT], block_recv.at[0, k // SPLIT], partner)

    def onward_copy(s, k):
        return remote(raw.at[s, piece(k), :], raw.at[s, piece(k), :],
                      send_sem.at[s, k // SPLIT], recv_sem.at[s - ONE, k], onward)

    def sent(lane, c):
        remote(raw.at[OWN, span(c), :], raw.at[OWN, span(c), :], send_sem.at[lane, c], block_recv.at[0, c], partner).wait_send()

    def send_own(first, last):
        @pl.when(role < 2)
        def _():
            for k in range(first, last):
                own_copy(k, recv_sem.at[own_slot - ONE, k]).start()

    def ids_copy(src, lane, slot, blk):
        return remote(src, idv.at[slot], ids_send.at[lane], ids_recv.at[slot], blk)

    @pl.when(has_own)
    def _():
        ids_copy(ids, 0, own_slot, own_to).start()

    send_own(0, SPLIT)

    @pl.when(role == 0)
    def _():
        send_own(SPLIT, pieces)

    @pl.when(gives_pair)
    def _():
        ids_copy(ids, 1, PAIR, partner).start()

    @pl.when(early)
    def _():
        for k in range(pieces):
            pair_copy(k).start()

    def normalize(values):
        values = values.astype(jnp.float32)
        scale = lax.rsqrt(jnp.sum(values * values, axis=-1, keepdims=True) + 1e-06)
        return (values * scale).astype(jnp.bfloat16)

    def ready(s, c):
        at = span(c)
        nrm[s, at, :] = normalize(raw[s, at, :])
        for p in range(ch // LANES):
            at = pl.ds(pl.multiple_of(c * ch + p * LANES, LANES), LANES)
            line = idv[s, :, at].astype(jnp.float32)
            idt[s, at, :] = jnp.transpose(jnp.broadcast_to(line, (LANES, LANES)))

    def tile(row, row_at, width, col, col_at):
        scores = lax.dot_general(
            nrm[col, col_at, :], nrm[row, row_at, :], (((1,), (1,)), ((), ())),
            preferred_element_type=jnp.float32)
        row_ids = idv[row, :, row_at].astype(jnp.float32)
        col_ids = idt[col, col_at, :]
        parts = []
        for p in range(width // LANES):
            cut = slice(p * LANES, (p + 1) * LANES)
            masked = jnp.where(col_ids < row_ids[:, cut], scores[:, cut], EMPTY)
            parts.append(jnp.max(masked, axis=0, keepdims=True))
        acc[row, :, row_at] = jnp.maximum(acc[row, :, row_at], jnp.concatenate(parts, axis=1))

    for s in range(1, 5):
        acc[s] = jnp.full((1, rows), EMPTY, jnp.float32)
    for copy in inputs:
        copy.wait()
    acc[OWN] = prior_v[...]
    local.wait()

    @pl.loop(0, CHUNKS)
    def _(c):
        ready(OWN, c)

    told(z == 1, 0, (0, g, b + 2))
    told(z == 2, 1, (1, g, b - 2))

    own_dev = owned.shape[0]
    owned_normed = normalize(owned_v[...])
    t_row = dest_v[...].astype(jnp.float32)
    t_col = jnp.transpose(jnp.broadcast_to(t_row, (LANES, own_dev)))[:, 0:1]
    row_i = lax.broadcasted_iota(jnp.int32, (own_dev, own_dev), 0)
    col_i = lax.broadcasted_iota(jnp.int32, (own_dev, own_dev), 1)
    earlier = jnp.where((row_i < col_i) & (t_col == t_row), 1.0, 0.0)
    position = jnp.sum(earlier, axis=0, keepdims=True)
    place = t_row * CAP + position
    which = lax.broadcasted_iota(jnp.int32, (devices * CAP, own_dev), 0).astype(jnp.float32)
    onehot = jnp.where(which == place, 1.0, 0.0).astype(jnp.bfloat16)
    outgoing = jnp.dot(onehot, owned_normed, preferred_element_type=jnp.float32).astype(jnp.bfloat16)
    dev_i = lax.broadcasted_iota(jnp.int32, (devices, own_dev), 0).astype(jnp.float32)
    lane_i = lax.broadcasted_iota(jnp.int32, (devices, LANES), 1)
    number = number_v[...].astype(jnp.float32) + 1.0
    outgoing_ids = jnp.full((devices, LANES), -1.0, jnp.float32)
    for k in range(CAP):
        here = jnp.where((dev_i == t_row) & (position == float(k)), number, 0.0)
        found = jnp.sum(here, axis=1, keepdims=True) - 1.0
        outgoing_ids = jnp.where(lane_i % CAP == k, found, outgoing_ids)
    outgoing_ids = outgoing_ids.astype(jnp.int32)
    for d in range(devices):
        obuf[d] = outgoing[d * CAP:(d + 1) * CAP, :]
        oid[d] = outgoing_ids[d:d + 1, :]

    told(z == 2, 0, (0, g, b + 2))
    told(z == 1, 1, (1, g, b - 2))

    keep_rows = pltpu.make_async_copy(obuf.at[me], rows_out.at[me], keep_sem.at[0])
    keep_ids = pltpu.make_async_copy(oid.at[me], ids_out.at[me], keep_sem.at[1])

    def start_routing():
        @pl.loop(1, devices)
        def _(step):
            other, og, ob = to_device(step)
            remote(obuf.at[other], rows_out.at[me], rows_send, rows_recv, ob, og).start()
            remote(oid.at[other], ids_out.at[me], oids_send, oids_recv, ob, og).start()

        keep_rows.start()
        keep_ids.start()

    def is_row(u, v):
        diff = (u - v + n_blk) % n_blk
        return (diff >= 1) & (diff <= CYCLE)

    slot_blocks = [b, partner, block_of(1), block_of(0), block_of(3)]

    def block_in(slot):
        result = slot_blocks[0]
        for i in range(1, 5):
            result = jnp.where(slot == i, slot_blocks[i], result)
        return result

    def run_units(table, phase, c):
        longest = max(len(entry) for by_phase in table for entry in by_phase)
        lists = [entry for by_phase in table for entry in by_phase]
        which_list = role * 2 + phase
        ends = [int(len(entry) > 0 and entry[-1] == OWN_PAIR) for entry in lists]
        count = pick(which_list, [len(entry) for entry in lists]) - pick(which_list, ends) * (1 - x)

        @pl.loop(0, count)
        def _(j):
            def entry(i):
                return pick(j * len(lists) + which_list,
                            [(lst[n] if n < len(lst) else (0, 0))[i] for n in range(longest) for lst in lists])

            u, v = entry(0), entry(1)
            bu, bv = block_in(u), block_in(v)

            @pl.when(is_row(bv, bu) | (u == v))
            def _():
                tile(v, whole, rows, u, span(c))

            @pl.when(is_row(bu, bv))
            def _():
                tile(u, span(c), ch, v, whole)

    def ids_wait(s):
        ids_copy(idv.at[s], 1, s, partner).wait_recv()

    def stream_wait(s, k):
        remote(raw.at[s, piece(k), :], raw.at[s, piece(k), :], send_sem.at[1, 0], recv_sem.at[s - ONE, k], partner).wait_recv()

    def block_wait(s, c):
        remote(raw.at[s, span(c), :], raw.at[s, span(c), :], send_sem.at[1, 0],
               block_recv.at[int(s == THREE), c], partner).wait_recv()

    def pass_on(s, k):
        stream_wait(s, k)

        @pl.when(role < 3)
        def _():
            onward_copy(s, k).start()

    def pass_ids(s):
        ids_wait(s)

        @pl.when(role < 3)
        def _():
            ids_copy(idv.at[s], s, s, onward).start()

    def take_three(c):
        @pl.when(c == 0)
        def _():
            ids_wait(THREE)

        block_wait(THREE, c)
        ready(THREE, c)

    @pl.when(role == 2)
    def _():
        pass_ids(ONE)
        for k in range(SPLIT):
            pass_on(ONE, k)

    @pl.loop(0, 2 * CHUNKS)
    def _(p):
        phase = p // CHUNKS
        c = p % CHUNKS
        has_in = (role > 0) & ((phase == 0) | (role > 1))
        s_in = jnp.where(phase == 0, ZERO, ONE)
        ahead = jnp.where((role == 2) & (phase == 1), 1, 0)
        c_in = (c + ahead) % CHUNKS

        def take(i):
            k = SPLIT * c_in + i

            if i == 0:
                @pl.when(has_in & (c == 0) & ((role != 2) | (phase == 0)))
                def _():
                    pass_ids(s_in)

            @pl.when(has_in & (c + ahead < CHUNKS))
            def _():
                pass_on(s_in, k)

            if i == SPLIT - 1:
                @pl.when((phase == 0) & (role == 0))
                def _():
                    sent(0, c)

            @pl.when((phase == 0) & (role == 3) & (k >= THREE_FROM) & (k < THREE_FROM + pieces // 2))
            def _():
                for n in range(2):
                    m = 2 * (k - THREE_FROM) + n
                    own_copy(m, block_recv.at[1, m // SPLIT]).start()

        @pl.when((phase == 1) & (role == 0) & gives_pair & (c > 0))
        def _():
            sent(1, c - 1)

        @pl.when((phase == 1) & (role < 2) & gives_pair & (c + LATE_LEAD < CHUNKS))
        def _():
            for i in range(SPLIT):
                pair_copy(SPLIT * (c + LATE_LEAD) + i).start()

        take(0)

        @pl.when((p == 2 * CHUNKS - 1) & (role == 3))
        def _():
            start_routing()

        @pl.when((role == 2) & (phase == 1))
        def _():
            take_three(c)

        run_units(UNITS[0], phase, c)
        take(1)

        @pl.when((p == LATE_STEP) & (role < 2) & gives_pair)
        def _():
            for k in range(LATE_LEAD * SPLIT):
                pair_copy(k).start()

        run_units(UNITS[1], phase, c)
        take(2)
        run_units(UNITS[2], phase, c)
        take(3)

        @pl.when((phase == 1) & (role < 2) & takes_pair)
        def _():
            @pl.when(c == 0)
            def _():
                ids_wait(PAIR)

            block_wait(PAIR, c)

        @pl.when((p == 2 * CHUNKS - 1) & (role == 0) & gives_pair)
        def _():
            sent(1, c)

        @pl.when((role < 3) & (p == jnp.where(role == 2, 2 * CHUNKS - 2, 2 * CHUNKS - 1)))
        def _():
            start_routing()

        @pl.when((p == CHUNKS - 1) & (role == 1))
        def _():
            send_own(SPLIT, pieces)

        told((p == 0) & (z == 3), 0)
        told((p == 0) & (z == 0), 1)
        told(p == 1, None, (2, other_core, b))
        told(p == 3, 2, (3, other_row, b))
        told(p == 4, 3)

        @pl.when(has_in)
        def _():
            ready(s_in, c_in)

        @pl.when((phase == 0) & early)
        def _():
            @pl.when(c == 0)
            def _():
                ids_wait(PAIR)

            block_wait(PAIR, c)

        @pl.when((early == (phase == 0)) & takes_pair)
        def _():
            ready(PAIR, c)

        run_units(UNITS[3], phase, c_in)

    def back(slot, index, r):
        return remote(acc.at[slot], ret.at[index], ret_send.at[slot], ret_recv.at[index],
                      partner if r is None else block_of(r))

    returns = [(role > 0, PAIR, 0, None), (role == 1, ZERO, 1, 0), (role == 2, ZERO, 2, 0), (role == 3, ZERO, 3, 0),
               (role == 2, ONE, 2, 1), (role == 3, ONE, 3, 1), (role == 2, THREE, 2, 3)]
    for when, slot, index, r in reversed(returns):
        @pl.when(when)
        def _(slot=slot, index=index, r=r):
            back(slot, index, r).start()

    own_result = pltpu.make_async_copy(acc.at[OWN], run_out, keep_sem.at[2])
    own_result.start()

    @pl.when(gives_pair)
    def _():
        ids_copy(ids, 1, PAIR, partner).wait_send()

    @pl.when(role > 0)
    def _():
        for c in range(CHUNKS):
            sent(1, c)

    @pl.when(has_own)
    def _():
        ids_copy(ids, 0, own_slot, own_to).wait_send()

    @pl.when((role == 1) | (role == 3))
    def _():
        for c in range(CHUNKS):
            sent(0, c)

    for s, sends in ((ONE, role == 2), (ZERO, (role == 1) | (role == 2))):
        @pl.when(sends)
        def _(s=s):
            ids_copy(idv.at[s], s, s, onward).wait_send()
            for c in range(CHUNKS):
                sent(s, c)

    own_result.wait()
    keep_rows.wait()
    keep_ids.wait()
    others = pl.ds(0, devices - 1)
    pltpu.make_async_copy(obuf.at[others], rows_out.at[others], rows_send).wait()
    pltpu.make_async_copy(oid.at[others], ids_out.at[others], oids_send).wait()
    pltpu.make_async_copy(obuf.at[others], rows_out.at[others], rows_recv).wait()
    pltpu.make_async_copy(oid.at[others], ids_out.at[others], oids_recv).wait()

    for index, gets in enumerate((role > 0, role == 0, (role != 2), role < 2)):
        @pl.when(gets)
        def _(index=index):
            remote(acc.at[PAIR], ret.at[index], ret_send.at[PAIR], ret_recv.at[index], partner).wait_recv()

    for when, slot, index, r in returns:
        @pl.when(when)
        def _(slot=slot, index=index, r=r):
            back(slot, index, r).wait_send()


def place_kernel(line, run, routed, routed_ids, *rest):
    if line:
        ret, run_out, rows_out, ids_out = rest
        z = lax.axis_index("blk") // 2
        role = z + (lax.axis_index("grp") % 2) * (3 - 2 * z)
        result = run[...]
        for index, gets in enumerate((role > 0, role == 0, role != 2, role < 2)):
            result = jnp.maximum(result, jnp.where(gets, ret[index], EMPTY))
        run_out[...] = result
    else:
        run_out, rows_out, ids_out = rest
        run_out[...] = run[...]
    devices, cap, _ = routed.shape
    for d in range(0, devices, 2):
        both = jnp.concatenate([routed[d].astype(jnp.float32), routed[d + 1].astype(jnp.float32)], axis=0)
        rows_out[d * cap:(d + 2) * cap, :] = both.astype(jnp.bfloat16)
    lines = routed_ids[...].reshape(devices, LANES)
    for part in range(devices * cap // LANES):
        sub = lines[part * LANES // cap:(part + 1) * LANES // cap, :]
        row_i = lax.broadcasted_iota(jnp.int32, sub.shape, 0)
        lane_i = lax.broadcasted_iota(jnp.int32, sub.shape, 1)
        mine = jnp.where(lane_i // cap == row_i, sub, 0)
        ids_out[:, part * LANES:(part + 1) * LANES] = jnp.sum(mine, axis=0, keepdims=True)


def body(embeds, doc_ids, prior_max, owned, owned_ids, owner_dest):
    n_grp, n_blk = lax.axis_size("grp"), lax.axis_size("blk")
    devices = n_grp * n_blk
    line = (n_grp, n_blk) == (4, 8)
    rows, width = embeds.shape[1:]
    own_dev = owned.shape[0]
    vmem = pl.BlockSpec(memory_space=pltpu.VMEM)
    anywhere = pl.BlockSpec(memory_space=pl.ANY)
    dma = pltpu.SemaphoreType.DMA
    shapes = (
        jax.ShapeDtypeStruct((1, rows), jnp.float32),
        jax.ShapeDtypeStruct((devices, CAP, width), jnp.bfloat16),
        jax.ShapeDtypeStruct((devices, 1, LANES), jnp.int32),
    )
    limit = 60 * 1024 * 1024
    if line:
        slots, pieces = 5, SPLIT * CHUNKS
        results = pl.pallas_call(
            functools.partial(line_kernel, (n_grp, n_blk)),
            out_shape=shapes + (jax.ShapeDtypeStruct((4, 1, rows), jnp.float32),),
            in_specs=[anywhere] * 6,
            out_specs=(anywhere,) * 4,
            scratch_shapes=[
                pltpu.VMEM((slots, rows, width), jnp.bfloat16),
                pltpu.VMEM((slots, rows, width), jnp.bfloat16),
                pltpu.VMEM((slots, 1, rows), jnp.int32),
                pltpu.VMEM((slots, rows, LANES), jnp.float32),
                pltpu.VMEM((slots, 1, rows), jnp.float32),
                pltpu.VMEM((devices, CAP, width), jnp.bfloat16),
                pltpu.VMEM((devices, 1, LANES), jnp.int32),
                pltpu.VMEM((1, rows), jnp.float32),
                pltpu.VMEM((own_dev, width), jnp.bfloat16),
                pltpu.VMEM((1, own_dev), jnp.int32),
                pltpu.VMEM((1, own_dev), jnp.int32),
                dma, dma((5,)), dma((4, CHUNKS)), dma((2, pieces)), dma((2, CHUNKS)),
                dma((slots,)), dma((slots,)), dma((slots,)), dma((4,)),
                dma, dma, dma, dma, dma((3,)), pltpu.SemaphoreType.REGULAR((4,)),
            ],
            compiler_params=pltpu.CompilerParams(has_side_effects=True, collective_id=0, vmem_limit_bytes=limit),
        )(embeds, doc_ids, prior_max, owned, owned_ids.reshape(1, own_dev), owner_dest.reshape(1, own_dev))
    else:
        plan = make_plan(n_blk // 2)
        received, returns = plan[0], plan[5]
        slots = max(len(entry) for entry in received)
        results = pl.pallas_call(
            functools.partial(ring_kernel, plan, (n_grp, n_blk)),
            out_shape=shapes,
            in_specs=[anywhere, vmem, vmem, vmem, vmem, vmem],
            out_specs=(vmem, anywhere, anywhere),
            scratch_shapes=[
                pltpu.VMEM((2 + slots, rows, width), jnp.bfloat16),
                pltpu.VMEM((2 + slots, rows, width), jnp.bfloat16),
                pltpu.VMEM((2 + slots, 1, rows), jnp.int32),
                pltpu.VMEM((2 + slots, rows, LANES), jnp.float32),
                pltpu.VMEM((2 + slots, 1, rows), jnp.float32),
                pltpu.VMEM((1 + max(returns), 1, rows), jnp.float32),
                pltpu.VMEM((devices, CAP, width), jnp.bfloat16),
                pltpu.VMEM((devices, 1, LANES), jnp.int32),
                dma, dma((2 + slots, CHUNKS)), dma((2 + slots, CHUNKS)),
                dma((2 + slots,)), dma((2 + slots,)),
                dma((1 + slots,)), dma((1 + max(returns),)),
                dma, dma, dma, dma, dma((2,)),
            ],
            compiler_params=pltpu.CompilerParams(has_side_effects=True, vmem_limit_bytes=limit),
        )(embeds, doc_ids, prior_max, owned, owned_ids.reshape(1, own_dev), owner_dest)
    running, next_rows, next_ids = pl.pallas_call(
        functools.partial(place_kernel, line),
        out_shape=(
            jax.ShapeDtypeStruct((1, rows), jnp.float32),
            jax.ShapeDtypeStruct((devices * CAP, width), jnp.bfloat16),
            jax.ShapeDtypeStruct((1, devices * CAP), jnp.int32),
        ),
        in_specs=[vmem] * len(results),
        out_specs=(vmem,) * 3,
    )(*results)
    return (running, next_rows, next_ids.reshape(devices * CAP))


def solution(mesh):
    return jax.shard_map(
        body,
        mesh=mesh,
        in_specs=(
            P("grp", "blk", None),
            P("grp", "blk"),
            P("grp", "blk"),
            P(("grp", "blk"), None),
            P(("grp", "blk")),
            P(("grp", "blk"), None),
        ),
        out_specs=(P("grp", "blk"), P(("grp", "blk"), None), P(("grp", "blk"))),
        check_vma=False,
    )
```

```python
import functools

import jax
import jax.numpy as jnp
from jax import lax
from jax.experimental import pallas as pl
from jax.experimental.pallas import tpu as pltpu
from jax.sharding import PartitionSpec as P

CYCLE = 3
CAP = 4
CHUNKS = 4
LANES = 128
EMPTY = -2.0


def make_plan(nz):
    received = [[((z - 1) % nz, (z - 1) % nz), ((z - 2) % nz, (z - 1) % nz)] for z in range(nz)]
    late = [False] * nz
    own_to = [(-1, 0)] * nz
    forward = [[(-1, 0)] * len(received[z]) for z in range(nz)]
    rank = [[0] * len(received[z]) for z in range(nz)]
    returns = [0] * nz
    for z in range(nz):
        for slot, (block, source) in enumerate(received[z]):
            if block == source:
                own_to[source] = (z, slot)
            else:
                held = [entry[0] for entry in received[source]].index(block)
                forward[source][held] = (z, slot)
            rank[z][slot] = returns[block]
            returns[block] += 1
    return received, own_to, late, forward, rank, returns


def pick(index, values):
    result = jnp.int32(values[0])
    for i in range(1, len(values)):
        if values[i] != values[0]:
            result = jnp.where(index == i, jnp.int32(values[i]), result)
    return result


def ring_kernel(plan, sizes, emb, ids, prior, owned, owned_ids, dest,
           run_out, rows_out, ids_out,
           raw, nrm, idv, idt, acc, ret, obuf, oid,
           local_sem, send_sem, recv_sem, ids_send, ids_recv, ret_send, ret_recv,
           rows_send, rows_recv, oids_send, oids_recv, keep_sem):
    n_grp, n_blk = sizes
    devices = n_grp * n_blk
    nz = n_blk // 2
    received, own_to, late, forward, rank, returns = plan
    slots = max(len(entry) for entry in received)
    rows = emb.shape[1]
    ch = rows // CHUNKS
    g = lax.axis_index("grp")
    b = lax.axis_index("blk")
    flip = g % 2
    z = b // 2
    x = b % 2
    role = z + flip * (nz - 1 - 2 * z)

    def block_of(zr):
        return 2 * (zr + flip * (nz - 1 - 2 * zr)) + x

    partner = b + 1 - 2 * x

    def table(values, slot=None, empty=0):
        if slot is None:
            return pick(role, values)
        return pick(role, [v[slot] if slot < len(v) else empty for v in values])

    own_z, own_slot = table([v[0] for v in own_to]), table([v[1] for v in own_to])
    is_late = table([int(v) for v in late])
    exists = [table([[1] * len(v) for v in received], s) for s in range(slots)]
    slot_z = [table([[e[0] for e in v] for v in received], s) for s in range(slots)]
    fwd_z = [table([[e[0] for e in v] for v in forward], s, -1) for s in range(slots)]
    fwd_slot = [table([[e[1] for e in v] for v in forward], s) for s in range(slots)]
    ranks = [table(rank, s) for s in range(slots)]
    n_returns = table(returns)
    blocks = [b, partner] + [block_of(slot_z[s]) for s in range(slots)]

    def span(c):
        if isinstance(c, int):
            return pl.ds(c * ch, ch)
        return pl.ds(pl.multiple_of(c * ch, ch), ch)

    def remote(src, dst, ssem, rsem, blk, grp=None):
        return pltpu.make_async_remote_copy(
            src_ref=src, dst_ref=dst, send_sem=ssem, recv_sem=rsem,
            device_id=(g if grp is None else grp, blk), device_id_type=pl.DeviceIdType.MESH)

    def chunk_copy(src, lane, to_slot, blk, c):
        return remote(src, raw.at[to_slot, span(c), :], send_sem.at[lane, c], recv_sem.at[to_slot, c], blk)

    def ids_copy(src, lane, to_slot, blk):
        return remote(src, idv.at[to_slot], ids_send.at[lane], ids_recv.at[to_slot], blk)

    def own_column(c):
        return chunk_copy(emb.at[0, span(c), :], 1, 2 + own_slot, block_of(own_z), c)

    def partner_copy(c):
        return chunk_copy(emb.at[0, span(c), :], 0, 1, partner, c)

    def forward_copy(s, c):
        return chunk_copy(raw.at[2 + s, span(c), :], 2 + s, 2 + fwd_slot[s], block_of(fwd_z[s]), c)

    def start_own_column():
        ids_copy(ids, 1, 2 + own_slot, block_of(own_z)).start()
        for c in range(CHUNKS):
            own_column(c).start()

    local = pltpu.make_async_copy(emb.at[0], raw.at[0], local_sem)
    local.start()

    @pl.when((own_z >= 0) & (is_late == 0))
    def _():
        start_own_column()

    ids_copy(ids, 0, 1, partner).start()
    for c in range(CHUNKS):
        partner_copy(c).start()

    def normalize(values):
        values = values.astype(jnp.float32)
        scale = lax.rsqrt(jnp.sum(values * values, axis=-1, keepdims=True) + 1e-06)
        return (values * scale).astype(jnp.bfloat16)

    own_dev = owned.shape[0]
    owned_normed = normalize(owned[...])
    t_col = dest[...].astype(jnp.float32)
    t_row = jnp.transpose(jnp.broadcast_to(t_col, (own_dev, LANES)))[0:1, :]
    row_i = lax.broadcasted_iota(jnp.int32, (own_dev, own_dev), 0)
    col_i = lax.broadcasted_iota(jnp.int32, (own_dev, own_dev), 1)
    earlier = jnp.where((row_i < col_i) & (t_col == t_row), 1.0, 0.0)
    position = jnp.sum(earlier, axis=0, keepdims=True)
    place = t_row * CAP + position
    which = lax.broadcasted_iota(jnp.int32, (devices * CAP, own_dev), 0).astype(jnp.float32)
    onehot = jnp.where(which == place, 1.0, 0.0).astype(jnp.bfloat16)
    outgoing = jnp.dot(onehot, owned_normed, preferred_element_type=jnp.float32).astype(jnp.bfloat16)
    dev_i = lax.broadcasted_iota(jnp.int32, (devices, own_dev), 0).astype(jnp.float32)
    lane_i = lax.broadcasted_iota(jnp.int32, (devices, LANES), 1)
    number = owned_ids[...].astype(jnp.float32) + 1.0
    outgoing_ids = jnp.full((devices, LANES), -1.0, jnp.float32)
    for k in range(CAP):
        here = jnp.where((dev_i == t_row) & (position == float(k)), number, 0.0)
        found = jnp.sum(here, axis=1, keepdims=True) - 1.0
        outgoing_ids = jnp.where(lane_i % CAP == k, found, outgoing_ids)
    outgoing_ids = outgoing_ids.astype(jnp.int32)
    for d in range(devices):
        obuf[d] = outgoing[d * CAP:(d + 1) * CAP, :]
        oid[d] = outgoing_ids[d:d + 1, :]

    def ready(s, c):
        at = span(c)
        nrm[s, at, :] = normalize(raw[s, at, :])
        for p in range(ch // LANES):
            at = pl.ds(pl.multiple_of(c * ch + p * LANES, LANES), LANES)
            line = idv[s, :, at].astype(jnp.float32)
            idt[s, at, :] = jnp.transpose(jnp.broadcast_to(line, (LANES, LANES)))

    def tile(row, row_at, width, col, col_at):
        scores = lax.dot_general(
            nrm[col, col_at, :], nrm[row, row_at, :], (((1,), (1,)), ((), ())),
            preferred_element_type=jnp.float32)
        row_ids = idv[row, :, row_at].astype(jnp.float32)
        col_ids = idt[col, col_at, :]
        parts = []
        for p in range(width // LANES):
            cut = slice(p * LANES, (p + 1) * LANES)
            masked = jnp.where(col_ids < row_ids[:, cut], scores[:, cut], EMPTY)
            parts.append(jnp.max(masked, axis=0, keepdims=True))
        acc[row, :, row_at] = jnp.maximum(acc[row, :, row_at], jnp.concatenate(parts, axis=1))

    whole = pl.ds(0, rows)

    acc[0] = prior[...]
    for s in range(1, 2 + slots):
        acc[s] = jnp.full((1, rows), EMPTY, jnp.float32)
    idv[0] = ids[...]
    local.wait()

    @pl.loop(0, CHUNKS)
    def _(c):
        ready(0, c)

    me = g * n_blk + b

    def to_device(step):
        other = (me + step) % devices
        return other, other // n_blk, other % n_blk

    @pl.loop(1, devices)
    def _(step):
        other, og, ob = to_device(step)
        remote(obuf.at[other], rows_out.at[me], rows_send, rows_recv, ob, og).start()
        remote(oid.at[other], ids_out.at[me], oids_send, oids_recv, ob, og).start()

    keep_rows = pltpu.make_async_copy(obuf.at[me], rows_out.at[me], keep_sem.at[0])
    keep_ids = pltpu.make_async_copy(oid.at[me], ids_out.at[me], keep_sem.at[1])
    keep_rows.start()
    keep_ids.start()

    def is_row(u, v):
        diff = (u - v + n_blk) % n_blk
        return (diff >= 1) & (diff <= CYCLE)

    def against_whole(s, c, other):
        @pl.when(is_row(blocks[s], blocks[other]))
        def _():
            tile(s, span(c), ch, other, whole)

        @pl.when(is_row(blocks[other], blocks[s]))
        def _():
            tile(other, whole, rows, s, span(c))

    def against_part(s, c, other, count):
        @pl.when(is_row(blocks[s], blocks[other]))
        def _():
            @pl.loop(0, count)
            def _(j):
                tile(s, span(c), ch, other, span(j))

        @pl.when(is_row(blocks[other], blocks[s]))
        def _():
            @pl.loop(0, count)
            def _(j):
                tile(other, span(j), ch, s, span(c))

    def arrive(s, c):
        chunk_copy(raw.at[s, span(c), :], 0, s, partner, c).wait_recv()

        @pl.when(c == 0)
        def _():
            ids_copy(idv.at[s], 0, s, partner).wait_recv()

        if s >= 2:
            @pl.when(fwd_z[s - 2] >= 0)
            def _():
                forward_copy(s - 2, c).start()

                @pl.when(c == 0)
                def _():
                    ids_copy(idv.at[s], s, 2 + fwd_slot[s - 2], block_of(fwd_z[s - 2])).start()

    @pl.loop(0, CHUNKS)
    def _(c):
        tile(0, whole, rows, 0, span(c))

    @pl.loop(0, CHUNKS)
    def _(c):
        @pl.when(exists[0] == 1)
        def _():
            arrive(2, c)
            ready(2, c)
            against_whole(2, c, 0)

    @pl.when((own_z >= 0) & (is_late == 1))
    def _():
        start_own_column()

    @pl.loop(0, CHUNKS)
    def _(c):
        for s in range(1, slots):
            @pl.when(exists[s] == 1)
            def _(s=s):
                arrive(2 + s, c)
                ready(2 + s, c)
                against_whole(2 + s, c, 0)
                against_part(2 + s, c, 1, c)

        arrive(1, c)
        ready(1, c)

        @pl.when(is_row(b, partner))
        def _():
            tile(0, whole, rows, 1, span(c))

        @pl.when(exists[0] == 1)
        def _():
            against_whole(1, c, 2)

        for s in range(1, slots):
            @pl.when(exists[s] == 1)
            def _(s=s):
                against_part(1, c, 2 + s, c + 1)

    back = remote(acc.at[1], ret.at[0], ret_send.at[0], ret_recv.at[0], partner)
    back.start()
    for s in range(slots):
        @pl.when(exists[s] == 1)
        def _(s=s):
            remote(acc.at[2 + s], ret.at[1 + ranks[s]], ret_send.at[1 + s], ret_recv.at[1 + ranks[s]],
                   block_of(slot_z[s])).start()

    for c in range(CHUNKS):
        partner_copy(c).wait_send()
    ids_copy(ids, 0, 1, partner).wait_send()

    @pl.when(own_z >= 0)
    def _():
        for c in range(CHUNKS):
            own_column(c).wait_send()
        ids_copy(ids, 1, 2 + own_slot, block_of(own_z)).wait_send()

    for s in range(slots):
        @pl.when(fwd_z[s] >= 0)
        def _(s=s):
            for c in range(CHUNKS):
                forward_copy(s, c).wait_send()
            ids_copy(idv.at[2 + s], 2 + s, 2 + fwd_slot[s], block_of(fwd_z[s])).wait_send()

    keep_rows.wait()
    keep_ids.wait()
    others = pl.ds(0, devices - 1)
    pltpu.make_async_copy(obuf.at[others], rows_out.at[others], rows_send).wait()
    pltpu.make_async_copy(oid.at[others], ids_out.at[others], oids_send).wait()
    pltpu.make_async_copy(obuf.at[others], rows_out.at[others], rows_recv).wait()
    pltpu.make_async_copy(oid.at[others], ids_out.at[others], oids_recv).wait()

    back.wait_recv()
    run_out[...] = jnp.maximum(acc[0], ret[0])
    for k in range(max(returns)):
        @pl.when(k < n_returns)
        def _(k=k):
            remote(acc.at[1], ret.at[1 + k], ret_send.at[0], ret_recv.at[1 + k], partner).wait_recv()
            run_out[...] = jnp.maximum(run_out[...], ret[1 + k])

    back.wait_send()
    for s in range(slots):
        @pl.when(exists[s] == 1)
        def _(s=s):
            remote(acc.at[2 + s], ret.at[1 + ranks[s]], ret_send.at[1 + s], ret_recv.at[1 + ranks[s]],
                   block_of(slot_z[s])).wait_send()


SPLIT = 4
LATE_LEAD = 2
LATE_STEP = 3
THREE_FROM = 7
OWN, PAIR, ONE, ZERO, THREE = range(5)
SELF_UNIT = (OWN, OWN)
OWN_PAIR = (PAIR, OWN)
KINDS = 3
UNITS = (
    (((), (), ()), ((), (), ()),
     ((), ((THREE, OWN),), ((ONE, OWN), (ONE, PAIR))), ((), (), ())),
    (((SELF_UNIT,), (), ()), ((SELF_UNIT,), (), ()),
     ((SELF_UNIT,), ((ZERO, PAIR),), ((ZERO, PAIR),)), ((SELF_UNIT,), ((ZERO, PAIR),), ((ZERO, PAIR),))),
    (((), (), ()), ((), (), ()),
     ((), ((THREE, PAIR),), ((THREE, OWN),)), ((), (), ())),
    (((), (OWN_PAIR,), (OWN_PAIR,)),
     (((ZERO, OWN),), ((PAIR, ZERO), OWN_PAIR), ((PAIR, ZERO), OWN_PAIR)),
     ((OWN_PAIR,), ((ONE, OWN), (ONE, PAIR)), ((THREE, PAIR),)),
     (((ZERO, OWN), OWN_PAIR), ((ONE, PAIR),), ((ONE, PAIR),))),
)


def line_kernel(sizes, emb, ids, prior, owned, owned_ids, dest,
                run_out, rows_out, ids_out, ret,
                raw, nrm, idv, idt, acc, obuf, oid, prior_v, owned_v, number_v, dest_v,
                local_sem, in_sem, send_sem, recv_sem, block_recv, ids_send, ids_recv, ret_send, ret_recv,
                rows_send, rows_recv, oids_send, oids_recv, keep_sem, known_sem):
    n_grp, n_blk = sizes
    devices = n_grp * n_blk
    rows = emb.shape[1]
    ch = rows // CHUNKS
    part = ch // SPLIT
    g = lax.axis_index("grp")
    b = lax.axis_index("blk")
    flip = g % 2
    z = b // 2
    x = b % 2
    role = z + flip * (3 - 2 * z)
    partner = b + 1 - 2 * x
    me = g * n_blk + b

    def block_of(r):
        return 2 * (r + flip * (3 - 2 * r)) + x

    def to_device(step):
        place = step - 1 + jnp.where(step > 2 * n_blk, 1, 0)
        turn = place // n_blk
        u = place % n_blk
        og = (g + u // 2) % n_grp
        oz = pick(4 * z + turn, [3, 2, 0, 1, 3, 2, 1, 0, 0, 1, 2, 3, 0, 1, 3, 2])
        ob = 2 * oz + (x + u) % 2
        return og * n_blk + ob, og, ob

    barrier = pltpu.get_barrier_semaphore()

    def signal(semaphore, grp, blk):
        pl.semaphore_signal(semaphore, inc=1, device_id=(grp, blk), device_id_type=pl.DeviceIdType.MESH)

    other_core = g + 1 - 2 * flip
    other_row = (g + n_grp // 2) % n_grp
    signal(barrier, g, partner)
    signal(barrier, other_core, b)
    signal(barrier, other_row, b)

    @pl.when(z > 0)
    def _():
        signal(barrier, g, b - 2)

    @pl.when(z < 3)
    def _():
        signal(barrier, g, b + 2)

    local = pltpu.make_async_copy(emb.at[0], raw.at[OWN], local_sem)
    local.start()
    inputs = [pltpu.make_async_copy(src, dst, in_sem.at[i]) for i, (src, dst) in enumerate((
        (ids, idv.at[OWN]), (prior, prior_v), (owned, owned_v), (owned_ids, number_v), (dest, dest_v)))]
    for copy in inputs:
        copy.start()

    pl.semaphore_wait(barrier, jnp.where((z == 1) | (z == 2), 5, 4))

    def told(here, index, then=None):
        @pl.when(here)
        def _():
            if index is not None:
                pl.semaphore_wait(known_sem.at[index], 1)
            if then is not None:
                signal(known_sem.at[then[0]], then[1], then[2])

    told(z == 0, None, (0, g, b + 2))
    told(z == 3, None, (1, g, b - 2))

    def remote(src, dst, ssem, rsem, blk, grp=None):
        return pltpu.make_async_remote_copy(
            src_ref=src, dst_ref=dst, send_sem=ssem, recv_sem=rsem,
            device_id=(g if grp is None else grp, blk), device_id_type=pl.DeviceIdType.MESH)

    def piece(k):
        if isinstance(k, int):
            return pl.ds(k * part, part)
        return pl.ds(pl.multiple_of(k * part, part), part)

    def span(c):
        if isinstance(c, int):
            return pl.ds(c * ch, ch)
        return pl.ds(pl.multiple_of(c * ch, ch), ch)

    whole = pl.ds(0, rows)
    pieces = SPLIT * CHUNKS

    own_slot = pick(role, [ZERO, ONE, ONE, THREE])
    own_to = block_of(pick(role, [1, 2, 3, 2]))
    has_own = role != 2
    onward = block_of(role + 1)
    gives_pair = (role > 0) | (x == 0)
    takes_pair = (role > 0) | (x == 1)
    early = role >= 2

    def own_copy(k, sem):
        return remote(emb.at[0, piece(k), :], raw.at[own_slot, piece(k), :],
                      send_sem.at[0, k // SPLIT], sem, own_to)

    def pair_copy(k):
        return remote(emb.at[0, piece(k), :], raw.at[PAIR, piece(k), :],
                      send_sem.at[1, k // SPLIT], block_recv.at[0, k // SPLIT], partner)

    def onward_copy(s, k):
        return remote(raw.at[s, piece(k), :], raw.at[s, piece(k), :],
                      send_sem.at[s, k // SPLIT], recv_sem.at[s - ONE, k], onward)

    def sent(lane, c):
        remote(raw.at[OWN, span(c), :], raw.at[OWN, span(c), :], send_sem.at[lane, c], block_recv.at[0, c], partner).wait_send()

    def send_own(first, last):
        @pl.when(role < 2)
        def _():
            for k in range(first, last):
                own_copy(k, recv_sem.at[own_slot - ONE, k]).start()

    def ids_copy(src, lane, slot, blk):
        return remote(src, idv.at[slot], ids_send.at[lane], ids_recv.at[slot], blk)

    @pl.when(has_own)
    def _():
        ids_copy(ids, 0, own_slot, own_to).start()

    send_own(0, SPLIT)

    @pl.when(role == 0)
    def _():
        send_own(SPLIT, pieces)

    @pl.when(gives_pair)
    def _():
        ids_copy(ids, 1, PAIR, partner).start()

    @pl.when(early)
    def _():
        for k in range(pieces):
            pair_copy(k).start()

    def normalize(values):
        values = values.astype(jnp.float32)
        scale = lax.rsqrt(jnp.sum(values * values, axis=-1, keepdims=True) + 1e-06)
        return (values * scale).astype(jnp.bfloat16)

    def ready(s, c):
        at = span(c)
        nrm[s, at, :] = normalize(raw[s, at, :])
        for p in range(ch // LANES):
            at = pl.ds(pl.multiple_of(c * ch + p * LANES, LANES), LANES)
            line = idv[s, :, at].astype(jnp.float32)
            idt[s, at, :] = jnp.transpose(jnp.broadcast_to(line, (LANES, LANES)))

    def tile(row, row_at, width, col, col_at):
        scores = lax.dot_general(
            nrm[col, col_at, :], nrm[row, row_at, :], (((1,), (1,)), ((), ())),
            preferred_element_type=jnp.float32)
        row_ids = idv[row, :, row_at].astype(jnp.float32)
        col_ids = idt[col, col_at, :]
        parts = []
        for p in range(width // LANES):
            cut = slice(p * LANES, (p + 1) * LANES)
            masked = jnp.where(col_ids < row_ids[:, cut], scores[:, cut], EMPTY)
            parts.append(jnp.max(masked, axis=0, keepdims=True))
        acc[row, :, row_at] = jnp.maximum(acc[row, :, row_at], jnp.concatenate(parts, axis=1))

    for s in range(1, 5):
        acc[s] = jnp.full((1, rows), EMPTY, jnp.float32)
    for copy in inputs:
        copy.wait()
    acc[OWN] = prior_v[...]
    local.wait()

    @pl.loop(0, CHUNKS)
    def _(c):
        ready(OWN, c)

    told(z == 1, 0, (0, g, b + 2))
    told(z == 2, 1, (1, g, b - 2))

    own_dev = owned.shape[0]
    owned_normed = normalize(owned_v[...])
    t_row = dest_v[...].astype(jnp.float32)
    t_col = jnp.transpose(jnp.broadcast_to(t_row, (LANES, own_dev)))[:, 0:1]
    row_i = lax.broadcasted_iota(jnp.int32, (own_dev, own_dev), 0)
    col_i = lax.broadcasted_iota(jnp.int32, (own_dev, own_dev), 1)
    earlier = jnp.where((row_i < col_i) & (t_col == t_row), 1.0, 0.0)
    position = jnp.sum(earlier, axis=0, keepdims=True)
    place = t_row * CAP + position
    which = lax.broadcasted_iota(jnp.int32, (devices * CAP, own_dev), 0).astype(jnp.float32)
    onehot = jnp.where(which == place, 1.0, 0.0).astype(jnp.bfloat16)
    outgoing = jnp.dot(onehot, owned_normed, preferred_element_type=jnp.float32).astype(jnp.bfloat16)
    dev_i = lax.broadcasted_iota(jnp.int32, (devices, own_dev), 0).astype(jnp.float32)
    lane_i = lax.broadcasted_iota(jnp.int32, (devices, LANES), 1)
    number = number_v[...].astype(jnp.float32) + 1.0
    outgoing_ids = jnp.full((devices, LANES), -1.0, jnp.float32)
    for k in range(CAP):
        here = jnp.where((dev_i == t_row) & (position == float(k)), number, 0.0)
        found = jnp.sum(here, axis=1, keepdims=True) - 1.0
        outgoing_ids = jnp.where(lane_i % CAP == k, found, outgoing_ids)
    outgoing_ids = outgoing_ids.astype(jnp.int32)
    for d in range(devices):
        obuf[d] = outgoing[d * CAP:(d + 1) * CAP, :]
        oid[d] = outgoing_ids[d:d + 1, :]

    told(z == 2, 0, (0, g, b + 2))
    told(z == 1, 1, (1, g, b - 2))

    keep_rows = pltpu.make_async_copy(obuf.at[me], rows_out.at[me], keep_sem.at[0])
    keep_ids = pltpu.make_async_copy(oid.at[me], ids_out.at[me], keep_sem.at[1])

    def start_routing(upward):
        @pl.loop(1, devices)
        def _(step):
            other, og, ob = to_device(step)

            @pl.when((ob // 2 > z) == upward)
            def _():
                remote(obuf.at[other], rows_out.at[me], rows_send, rows_recv, ob, og).start()
                remote(oid.at[other], ids_out.at[me], oids_send, oids_recv, ob, og).start()

        if not upward:
            keep_rows.start()
            keep_ids.start()

    def is_row(u, v):
        diff = (u - v + n_blk) % n_blk
        return (diff >= 1) & (diff <= CYCLE)

    slot_blocks = [b, partner, block_of(1), block_of(0), block_of(3)]

    def block_in(slot):
        result = slot_blocks[0]
        for i in range(1, 5):
            result = jnp.where(slot == i, slot_blocks[i], result)
        return result

    def run_units(table, kind, c):
        longest = max(len(entry) for by_phase in table for entry in by_phase)
        lists = [entry for by_phase in table for entry in by_phase]
        which_list = role * KINDS + kind
        ends = [int(len(entry) > 0 and entry[-1] == OWN_PAIR) for entry in lists]
        count = pick(which_list, [len(entry) for entry in lists]) - pick(which_list, ends) * (1 - x)

        @pl.loop(0, count)
        def _(j):
            def entry(i):
                return pick(j * len(lists) + which_list,
                            [(lst[n] if n < len(lst) else (0, 0))[i] for n in range(longest) for lst in lists])

            u, v = entry(0), entry(1)
            bu, bv = block_in(u), block_in(v)

            @pl.when(is_row(bv, bu) | (u == v))
            def _():
                tile(v, whole, rows, u, span(c))

            @pl.when(is_row(bu, bv))
            def _():
                tile(u, span(c), ch, v, whole)

    def ids_wait(s):
        ids_copy(idv.at[s], 1, s, partner).wait_recv()

    def stream_wait(s, k):
        remote(raw.at[s, piece(k), :], raw.at[s, piece(k), :], send_sem.at[1, 0], recv_sem.at[s - ONE, k], partner).wait_recv()

    def block_wait(s, c):
        remote(raw.at[s, span(c), :], raw.at[s, span(c), :], send_sem.at[1, 0],
               block_recv.at[int(s == THREE), c], partner).wait_recv()

    def back(slot, index, r):
        return remote(acc.at[slot], ret.at[index], ret_send.at[slot], ret_recv.at[index],
                      partner if r is None else block_of(r))

    def pass_on(s, k):
        stream_wait(s, k)

        @pl.when(role < 3)
        def _():
            onward_copy(s, k).start()

    def pass_ids(s):
        ids_wait(s)

        @pl.when(role < 3)
        def _():
            ids_copy(idv.at[s], s, s, onward).start()

    def take_three(c):
        @pl.when(c == 0)
        def _():
            ids_wait(THREE)

        block_wait(THREE, c)
        ready(THREE, c)

    @pl.when(role == 2)
    def _():
        pass_ids(ONE)
        for k in range(SPLIT):
            pass_on(ONE, k)
        ready(ONE, jnp.int32(0))

    @pl.loop(0, 2 * CHUNKS)
    def _(p):
        phase = p // CHUNKS
        c = p % CHUNKS
        has_in = (role > 0) & ((phase == 0) | (role > 1))
        s_in = jnp.where(phase == 0, ZERO, ONE)
        ahead = jnp.where((role == 2) & (phase == 1), 1, 0)
        c_in = (c + ahead) % CHUNKS
        last = p == 2 * CHUNKS - 1
        kind = phase + jnp.where(last, 1, 0)

        def take(i):
            k = SPLIT * c_in + i

            if i == 0:
                @pl.when(has_in & (c == 0) & ((role != 2) | (phase == 0)))
                def _():
                    pass_ids(s_in)

            @pl.when(has_in & (c + ahead < CHUNKS))
            def _():
                pass_on(s_in, k)

            if i == SPLIT - 1:
                @pl.when((phase == 0) & (role == 0))
                def _():
                    sent(0, c)

            @pl.when((phase == 0) & (role == 3) & (k >= THREE_FROM) & (k < THREE_FROM + pieces // 2))
            def _():
                for n in range(2):
                    m = 2 * (k - THREE_FROM) + n
                    own_copy(m, block_recv.at[1, m // SPLIT]).start()

        @pl.when((phase == 1) & (role == 0) & gives_pair & (c > 0))
        def _():
            sent(1, c - 1)

        @pl.when((phase == 1) & (role < 2) & gives_pair & (c + LATE_LEAD < CHUNKS))
        def _():
            for i in range(SPLIT):
                pair_copy(SPLIT * (c + LATE_LEAD) + i).start()

        take(0)

        @pl.when((p == 2 * CHUNKS - 1) & (role == 3))
        def _():
            start_routing(False)

        @pl.when((role == 2) & (phase == 1))
        def _():
            take_three(c)

        run_units(UNITS[0], kind, jnp.where(last, c_in, c))

        @pl.when(last & (role == 2))
        def _():
            back(ONE, 2, 1).start()

        take(1)

        @pl.when((p == LATE_STEP) & (role < 2) & gives_pair)
        def _():
            for k in range(LATE_LEAD * SPLIT):
                pair_copy(k).start()

        run_units(UNITS[1], kind, c)

        @pl.when((p == 2 * CHUNKS - 1) & early)
        def _():
            back(ZERO, role, 0).start()
            start_routing(True)

        take(2)
        run_units(UNITS[2], kind, c)
        take(3)

        @pl.when((phase == 1) & (role < 2) & takes_pair)
        def _():
            @pl.when(c == 0)
            def _():
                ids_wait(PAIR)

            block_wait(PAIR, c)

        @pl.when((p == 2 * CHUNKS - 1) & (role == 0) & gives_pair)
        def _():
            sent(1, c)

        @pl.when((role < 3) & (p == jnp.where(role == 2, 2 * CHUNKS - 2, 2 * CHUNKS - 1)))
        def _():
            start_routing(False)

        @pl.when((p == CHUNKS - 1) & (role == 1))
        def _():
            send_own(SPLIT, pieces)

        told((p == 0) & (z == 3), 0)
        told((p == 0) & (z == 0), 1)
        told(p == 1, None, (2, other_core, b))
        told(p == 3, 2, (3, other_row, b))
        told(p == 4, 3)

        @pl.when(has_in & (c + ahead < CHUNKS))
        def _():
            ready(s_in, c_in)

        @pl.when((phase == 0) & early)
        def _():
            @pl.when(c == 0)
            def _():
                ids_wait(PAIR)

            block_wait(PAIR, c)

        @pl.when((early == (phase == 0)) & takes_pair)
        def _():
            ready(PAIR, c)

        run_units(UNITS[3], kind, jnp.where(last, c, c_in))

    returns = [(role > 0, PAIR, 0, None), (role == 1, ZERO, 1, 0), (role == 2, ZERO, 2, 0), (role == 3, ZERO, 3, 0),
               (role == 2, ONE, 2, 1), (role == 3, ONE, 3, 1), (role == 2, THREE, 2, 3)]
    for when, slot, index, r in reversed(returns):
        if (slot == ZERO and index > 1) or (slot, index) == (ONE, 2):
            continue

        @pl.when(when)
        def _(slot=slot, index=index, r=r):
            back(slot, index, r).start()

    def returned(index):
        remote(acc.at[PAIR], ret.at[index], ret_send.at[PAIR], ret_recv.at[index], partner).wait_recv()

    @pl.when(role < 2)
    def _():
        start_routing(True)

    own_result = pltpu.make_async_copy(acc.at[OWN], run_out, keep_sem.at[2])
    own_result.start()

    @pl.when(gives_pair)
    def _():
        ids_copy(ids, 1, PAIR, partner).wait_send()

    @pl.when(role > 0)
    def _():
        for c in range(CHUNKS):
            sent(1, c)

    @pl.when(has_own)
    def _():
        ids_copy(ids, 0, own_slot, own_to).wait_send()

    @pl.when((role == 1) | (role == 3))
    def _():
        for c in range(CHUNKS):
            sent(0, c)

    for s, sends in ((ONE, role == 2), (ZERO, (role == 1) | (role == 2))):
        @pl.when(sends)
        def _(s=s):
            ids_copy(idv.at[s], s, s, onward).wait_send()
            for c in range(CHUNKS):
                sent(s, c)

    own_result.wait()
    keep_rows.wait()
    keep_ids.wait()
    others = pl.ds(0, devices - 1)
    pltpu.make_async_copy(obuf.at[others], rows_out.at[others], rows_send).wait()
    pltpu.make_async_copy(oid.at[others], ids_out.at[others], oids_send).wait()
    pltpu.make_async_copy(obuf.at[others], rows_out.at[others], rows_recv).wait()
    pltpu.make_async_copy(oid.at[others], ids_out.at[others], oids_recv).wait()

    for index, gets in ((0, role > 0), (1, role == 0), (2, role != 2), (3, role < 2)):
        @pl.when(gets)
        def _(index=index):
            returned(index)

    for when, slot, index, r in returns:
        @pl.when(when)
        def _(slot=slot, index=index, r=r):
            back(slot, index, r).wait_send()


def place_kernel(line, run, routed, routed_ids, *rest):
    if line:
        ret, run_out, rows_out, ids_out = rest
        z = lax.axis_index("blk") // 2
        role = z + (lax.axis_index("grp") % 2) * (3 - 2 * z)
        result = run[...]
        for index, gets in enumerate((role > 0, role == 0, role != 2, role < 2)):
            result = jnp.maximum(result, jnp.where(gets, ret[index], EMPTY))
        run_out[...] = result
    else:
        run_out, rows_out, ids_out = rest
        run_out[...] = run[...]
    devices, cap, _ = routed.shape
    for d in range(0, devices, 2):
        both = jnp.concatenate([routed[d].astype(jnp.float32), routed[d + 1].astype(jnp.float32)], axis=0)
        rows_out[d * cap:(d + 2) * cap, :] = both.astype(jnp.bfloat16)
    lines = routed_ids[...].reshape(devices, LANES)
    for part in range(devices * cap // LANES):
        sub = lines[part * LANES // cap:(part + 1) * LANES // cap, :]
        row_i = lax.broadcasted_iota(jnp.int32, sub.shape, 0)
        lane_i = lax.broadcasted_iota(jnp.int32, sub.shape, 1)
        mine = jnp.where(lane_i // cap == row_i, sub, 0)
        ids_out[:, part * LANES:(part + 1) * LANES] = jnp.sum(mine, axis=0, keepdims=True)


def body(embeds, doc_ids, prior_max, owned, owned_ids, owner_dest):
    n_grp, n_blk = lax.axis_size("grp"), lax.axis_size("blk")
    devices = n_grp * n_blk
    line = (n_grp, n_blk) == (4, 8)
    rows, width = embeds.shape[1:]
    own_dev = owned.shape[0]
    vmem = pl.BlockSpec(memory_space=pltpu.VMEM)
    anywhere = pl.BlockSpec(memory_space=pl.ANY)
    dma = pltpu.SemaphoreType.DMA
    shapes = (
        jax.ShapeDtypeStruct((1, rows), jnp.float32),
        jax.ShapeDtypeStruct((devices, CAP, width), jnp.bfloat16),
        jax.ShapeDtypeStruct((devices, 1, LANES), jnp.int32),
    )
    limit = 60 * 1024 * 1024
    if line:
        slots, pieces = 5, SPLIT * CHUNKS
        results = pl.pallas_call(
            functools.partial(line_kernel, (n_grp, n_blk)),
            out_shape=shapes + (jax.ShapeDtypeStruct((4, 1, rows), jnp.float32),),
            in_specs=[anywhere] * 6,
            out_specs=(anywhere,) * 4,
            scratch_shapes=[
                pltpu.VMEM((slots, rows, width), jnp.bfloat16),
                pltpu.VMEM((slots, rows, width), jnp.bfloat16),
                pltpu.VMEM((slots, 1, rows), jnp.int32),
                pltpu.VMEM((slots, rows, LANES), jnp.float32),
                pltpu.VMEM((slots, 1, rows), jnp.float32),
                pltpu.VMEM((devices, CAP, width), jnp.bfloat16),
                pltpu.VMEM((devices, 1, LANES), jnp.int32),
                pltpu.VMEM((1, rows), jnp.float32),
                pltpu.VMEM((own_dev, width), jnp.bfloat16),
                pltpu.VMEM((1, own_dev), jnp.int32),
                pltpu.VMEM((1, own_dev), jnp.int32),
                dma, dma((5,)), dma((4, CHUNKS)), dma((2, pieces)), dma((2, CHUNKS)),
                dma((slots,)), dma((slots,)), dma((slots,)), dma((4,)),
                dma, dma, dma, dma, dma((3,)), pltpu.SemaphoreType.REGULAR((4,)),
            ],
            compiler_params=pltpu.CompilerParams(has_side_effects=True, collective_id=0, vmem_limit_bytes=limit),
        )(embeds, doc_ids, prior_max, owned, owned_ids.reshape(1, own_dev), owner_dest.reshape(1, own_dev))
    else:
        plan = make_plan(n_blk // 2)
        received, returns = plan[0], plan[5]
        slots = max(len(entry) for entry in received)
        results = pl.pallas_call(
            functools.partial(ring_kernel, plan, (n_grp, n_blk)),
            out_shape=shapes,
            in_specs=[anywhere, vmem, vmem, vmem, vmem, vmem],
            out_specs=(vmem, anywhere, anywhere),
            scratch_shapes=[
                pltpu.VMEM((2 + slots, rows, width), jnp.bfloat16),
                pltpu.VMEM((2 + slots, rows, width), jnp.bfloat16),
                pltpu.VMEM((2 + slots, 1, rows), jnp.int32),
                pltpu.VMEM((2 + slots, rows, LANES), jnp.float32),
                pltpu.VMEM((2 + slots, 1, rows), jnp.float32),
                pltpu.VMEM((1 + max(returns), 1, rows), jnp.float32),
                pltpu.VMEM((devices, CAP, width), jnp.bfloat16),
                pltpu.VMEM((devices, 1, LANES), jnp.int32),
                dma, dma((2 + slots, CHUNKS)), dma((2 + slots, CHUNKS)),
                dma((2 + slots,)), dma((2 + slots,)),
                dma((1 + slots,)), dma((1 + max(returns),)),
                dma, dma, dma, dma, dma((2,)),
            ],
            compiler_params=pltpu.CompilerParams(has_side_effects=True, vmem_limit_bytes=limit),
        )(embeds, doc_ids, prior_max, owned, owned_ids.reshape(1, own_dev), owner_dest)
    running, next_rows, next_ids = pl.pallas_call(
        functools.partial(place_kernel, line),
        out_shape=(
            jax.ShapeDtypeStruct((1, rows), jnp.float32),
            jax.ShapeDtypeStruct((devices * CAP, width), jnp.bfloat16),
            jax.ShapeDtypeStruct((1, devices * CAP), jnp.int32),
        ),
        in_specs=[vmem] * len(results),
        out_specs=(vmem,) * 3,
    )(*results)
    return (running, next_rows, next_ids.reshape(devices * CAP))


def solution(mesh):
    return jax.shard_map(
        body,
        mesh=mesh,
        in_specs=(
            P("grp", "blk", None),
            P("grp", "blk"),
            P("grp", "blk"),
            P(("grp", "blk"), None),
            P(("grp", "blk")),
            P(("grp", "blk"), None),
        ),
        out_specs=(P("grp", "blk"), P(("grp", "blk"), None), P(("grp", "blk"))),
        check_vma=False,
    )
```

```python
import functools

import jax
import jax.numpy as jnp
from jax import lax
from jax.experimental import pallas as pl
from jax.experimental.pallas import tpu as pltpu
from jax.sharding import PartitionSpec as P

CYCLE = 3
CAP = 4
CHUNKS = 4
LANES = 128
EMPTY = -2.0


def make_plan(nz):
    received = [[((z - 1) % nz, (z - 1) % nz), ((z - 2) % nz, (z - 1) % nz)] for z in range(nz)]
    late = [False] * nz
    own_to = [(-1, 0)] * nz
    forward = [[(-1, 0)] * len(received[z]) for z in range(nz)]
    rank = [[0] * len(received[z]) for z in range(nz)]
    returns = [0] * nz
    for z in range(nz):
        for slot, (block, source) in enumerate(received[z]):
            if block == source:
                own_to[source] = (z, slot)
            else:
                held = [entry[0] for entry in received[source]].index(block)
                forward[source][held] = (z, slot)
            rank[z][slot] = returns[block]
            returns[block] += 1
    return received, own_to, late, forward, rank, returns


def pick(index, values):
    result = jnp.int32(values[0])
    for i in range(1, len(values)):
        if values[i] != values[0]:
            result = jnp.where(index == i, jnp.int32(values[i]), result)
    return result


def ring_kernel(plan, sizes, emb, ids, prior, owned, owned_ids, dest,
           run_out, rows_out, ids_out,
           raw, nrm, idv, idt, acc, ret, obuf, oid,
           local_sem, send_sem, recv_sem, ids_send, ids_recv, ret_send, ret_recv,
           rows_send, rows_recv, oids_send, oids_recv, keep_sem):
    n_grp, n_blk = sizes
    devices = n_grp * n_blk
    nz = n_blk // 2
    received, own_to, late, forward, rank, returns = plan
    slots = max(len(entry) for entry in received)
    rows = emb.shape[1]
    ch = rows // CHUNKS
    g = lax.axis_index("grp")
    b = lax.axis_index("blk")
    flip = g % 2
    z = b // 2
    x = b % 2
    role = z + flip * (nz - 1 - 2 * z)

    def block_of(zr):
        return 2 * (zr + flip * (nz - 1 - 2 * zr)) + x

    partner = b + 1 - 2 * x

    def table(values, slot=None, empty=0):
        if slot is None:
            return pick(role, values)
        return pick(role, [v[slot] if slot < len(v) else empty for v in values])

    own_z, own_slot = table([v[0] for v in own_to]), table([v[1] for v in own_to])
    is_late = table([int(v) for v in late])
    exists = [table([[1] * len(v) for v in received], s) for s in range(slots)]
    slot_z = [table([[e[0] for e in v] for v in received], s) for s in range(slots)]
    fwd_z = [table([[e[0] for e in v] for v in forward], s, -1) for s in range(slots)]
    fwd_slot = [table([[e[1] for e in v] for v in forward], s) for s in range(slots)]
    ranks = [table(rank, s) for s in range(slots)]
    n_returns = table(returns)
    blocks = [b, partner] + [block_of(slot_z[s]) for s in range(slots)]

    def span(c):
        if isinstance(c, int):
            return pl.ds(c * ch, ch)
        return pl.ds(pl.multiple_of(c * ch, ch), ch)

    def remote(src, dst, ssem, rsem, blk, grp=None):
        return pltpu.make_async_remote_copy(
            src_ref=src, dst_ref=dst, send_sem=ssem, recv_sem=rsem,
            device_id=(g if grp is None else grp, blk), device_id_type=pl.DeviceIdType.MESH)

    def chunk_copy(src, lane, to_slot, blk, c):
        return remote(src, raw.at[to_slot, span(c), :], send_sem.at[lane, c], recv_sem.at[to_slot, c], blk)

    def ids_copy(src, lane, to_slot, blk):
        return remote(src, idv.at[to_slot], ids_send.at[lane], ids_recv.at[to_slot], blk)

    def own_column(c):
        return chunk_copy(emb.at[0, span(c), :], 1, 2 + own_slot, block_of(own_z), c)

    def partner_copy(c):
        return chunk_copy(emb.at[0, span(c), :], 0, 1, partner, c)

    def forward_copy(s, c):
        return chunk_copy(raw.at[2 + s, span(c), :], 2 + s, 2 + fwd_slot[s], block_of(fwd_z[s]), c)

    def start_own_column():
        ids_copy(ids, 1, 2 + own_slot, block_of(own_z)).start()
        for c in range(CHUNKS):
            own_column(c).start()

    local = pltpu.make_async_copy(emb.at[0], raw.at[0], local_sem)
    local.start()

    @pl.when((own_z >= 0) & (is_late == 0))
    def _():
        start_own_column()

    ids_copy(ids, 0, 1, partner).start()
    for c in range(CHUNKS):
        partner_copy(c).start()

    def normalize(values):
        values = values.astype(jnp.float32)
        scale = lax.rsqrt(jnp.sum(values * values, axis=-1, keepdims=True) + 1e-06)
        return (values * scale).astype(jnp.bfloat16)

    own_dev = owned.shape[0]
    owned_normed = normalize(owned[...])
    t_col = dest[...].astype(jnp.float32)
    t_row = jnp.transpose(jnp.broadcast_to(t_col, (own_dev, LANES)))[0:1, :]
    row_i = lax.broadcasted_iota(jnp.int32, (own_dev, own_dev), 0)
    col_i = lax.broadcasted_iota(jnp.int32, (own_dev, own_dev), 1)
    earlier = jnp.where((row_i < col_i) & (t_col == t_row), 1.0, 0.0)
    position = jnp.sum(earlier, axis=0, keepdims=True)
    place = t_row * CAP + position
    which = lax.broadcasted_iota(jnp.int32, (devices * CAP, own_dev), 0).astype(jnp.float32)
    onehot = jnp.where(which == place, 1.0, 0.0).astype(jnp.bfloat16)
    outgoing = jnp.dot(onehot, owned_normed, preferred_element_type=jnp.float32).astype(jnp.bfloat16)
    dev_i = lax.broadcasted_iota(jnp.int32, (devices, own_dev), 0).astype(jnp.float32)
    lane_i = lax.broadcasted_iota(jnp.int32, (devices, LANES), 1)
    number = owned_ids[...].astype(jnp.float32) + 1.0
    outgoing_ids = jnp.full((devices, LANES), -1.0, jnp.float32)
    for k in range(CAP):
        here = jnp.where((dev_i == t_row) & (position == float(k)), number, 0.0)
        found = jnp.sum(here, axis=1, keepdims=True) - 1.0
        outgoing_ids = jnp.where(lane_i % CAP == k, found, outgoing_ids)
    outgoing_ids = outgoing_ids.astype(jnp.int32)
    for d in range(devices):
        obuf[d] = outgoing[d * CAP:(d + 1) * CAP, :]
        oid[d] = outgoing_ids[d:d + 1, :]

    def ready(s, c):
        at = span(c)
        nrm[s, at, :] = normalize(raw[s, at, :])
        for p in range(ch // LANES):
            at = pl.ds(pl.multiple_of(c * ch + p * LANES, LANES), LANES)
            line = idv[s, :, at].astype(jnp.float32)
            idt[s, at, :] = jnp.transpose(jnp.broadcast_to(line, (LANES, LANES)))

    def tile(row, row_at, width, col, col_at):
        scores = lax.dot_general(
            nrm[col, col_at, :], nrm[row, row_at, :], (((1,), (1,)), ((), ())),
            preferred_element_type=jnp.float32)
        row_ids = idv[row, :, row_at].astype(jnp.float32)
        col_ids = idt[col, col_at, :]
        parts = []
        for p in range(width // LANES):
            cut = slice(p * LANES, (p + 1) * LANES)
            masked = jnp.where(col_ids < row_ids[:, cut], scores[:, cut], EMPTY)
            parts.append(jnp.max(masked, axis=0, keepdims=True))
        acc[row, :, row_at] = jnp.maximum(acc[row, :, row_at], jnp.concatenate(parts, axis=1))

    whole = pl.ds(0, rows)

    acc[0] = prior[...]
    for s in range(1, 2 + slots):
        acc[s] = jnp.full((1, rows), EMPTY, jnp.float32)
    idv[0] = ids[...]
    local.wait()

    @pl.loop(0, CHUNKS)
    def _(c):
        ready(0, c)

    me = g * n_blk + b

    def to_device(step):
        other = (me + step) % devices
        return other, other // n_blk, other % n_blk

    @pl.loop(1, devices)
    def _(step):
        other, og, ob = to_device(step)
        remote(obuf.at[other], rows_out.at[me], rows_send, rows_recv, ob, og).start()
        remote(oid.at[other], ids_out.at[me], oids_send, oids_recv, ob, og).start()

    keep_rows = pltpu.make_async_copy(obuf.at[me], rows_out.at[me], keep_sem.at[0])
    keep_ids = pltpu.make_async_copy(oid.at[me], ids_out.at[me], keep_sem.at[1])
    keep_rows.start()
    keep_ids.start()

    def is_row(u, v):
        diff = (u - v + n_blk) % n_blk
        return (diff >= 1) & (diff <= CYCLE)

    def against_whole(s, c, other):
        @pl.when(is_row(blocks[s], blocks[other]))
        def _():
            tile(s, span(c), ch, other, whole)

        @pl.when(is_row(blocks[other], blocks[s]))
        def _():
            tile(other, whole, rows, s, span(c))

    def against_part(s, c, other, count):
        @pl.when(is_row(blocks[s], blocks[other]))
        def _():
            @pl.loop(0, count)
            def _(j):
                tile(s, span(c), ch, other, span(j))

        @pl.when(is_row(blocks[other], blocks[s]))
        def _():
            @pl.loop(0, count)
            def _(j):
                tile(other, span(j), ch, s, span(c))

    def arrive(s, c):
        chunk_copy(raw.at[s, span(c), :], 0, s, partner, c).wait_recv()

        @pl.when(c == 0)
        def _():
            ids_copy(idv.at[s], 0, s, partner).wait_recv()

        if s >= 2:
            @pl.when(fwd_z[s - 2] >= 0)
            def _():
                forward_copy(s - 2, c).start()

                @pl.when(c == 0)
                def _():
                    ids_copy(idv.at[s], s, 2 + fwd_slot[s - 2], block_of(fwd_z[s - 2])).start()

    @pl.loop(0, CHUNKS)
    def _(c):
        tile(0, whole, rows, 0, span(c))

    @pl.loop(0, CHUNKS)
    def _(c):
        @pl.when(exists[0] == 1)
        def _():
            arrive(2, c)
            ready(2, c)
            against_whole(2, c, 0)

    @pl.when((own_z >= 0) & (is_late == 1))
    def _():
        start_own_column()

    @pl.loop(0, CHUNKS)
    def _(c):
        for s in range(1, slots):
            @pl.when(exists[s] == 1)
            def _(s=s):
                arrive(2 + s, c)
                ready(2 + s, c)
                against_whole(2 + s, c, 0)
                against_part(2 + s, c, 1, c)

        arrive(1, c)
        ready(1, c)

        @pl.when(is_row(b, partner))
        def _():
            tile(0, whole, rows, 1, span(c))

        @pl.when(exists[0] == 1)
        def _():
            against_whole(1, c, 2)

        for s in range(1, slots):
            @pl.when(exists[s] == 1)
            def _(s=s):
                against_part(1, c, 2 + s, c + 1)

    back = remote(acc.at[1], ret.at[0], ret_send.at[0], ret_recv.at[0], partner)
    back.start()
    for s in range(slots):
        @pl.when(exists[s] == 1)
        def _(s=s):
            remote(acc.at[2 + s], ret.at[1 + ranks[s]], ret_send.at[1 + s], ret_recv.at[1 + ranks[s]],
                   block_of(slot_z[s])).start()

    for c in range(CHUNKS):
        partner_copy(c).wait_send()
    ids_copy(ids, 0, 1, partner).wait_send()

    @pl.when(own_z >= 0)
    def _():
        for c in range(CHUNKS):
            own_column(c).wait_send()
        ids_copy(ids, 1, 2 + own_slot, block_of(own_z)).wait_send()

    for s in range(slots):
        @pl.when(fwd_z[s] >= 0)
        def _(s=s):
            for c in range(CHUNKS):
                forward_copy(s, c).wait_send()
            ids_copy(idv.at[2 + s], 2 + s, 2 + fwd_slot[s], block_of(fwd_z[s])).wait_send()

    keep_rows.wait()
    keep_ids.wait()
    others = pl.ds(0, devices - 1)
    pltpu.make_async_copy(obuf.at[others], rows_out.at[others], rows_send).wait()
    pltpu.make_async_copy(oid.at[others], ids_out.at[others], oids_send).wait()
    pltpu.make_async_copy(obuf.at[others], rows_out.at[others], rows_recv).wait()
    pltpu.make_async_copy(oid.at[others], ids_out.at[others], oids_recv).wait()

    back.wait_recv()
    run_out[...] = jnp.maximum(acc[0], ret[0])
    for k in range(max(returns)):
        @pl.when(k < n_returns)
        def _(k=k):
            remote(acc.at[1], ret.at[1 + k], ret_send.at[0], ret_recv.at[1 + k], partner).wait_recv()
            run_out[...] = jnp.maximum(run_out[...], ret[1 + k])

    back.wait_send()
    for s in range(slots):
        @pl.when(exists[s] == 1)
        def _(s=s):
            remote(acc.at[2 + s], ret.at[1 + ranks[s]], ret_send.at[1 + s], ret_recv.at[1 + ranks[s]],
                   block_of(slot_z[s])).wait_send()


SPLIT = 4
LATE_LEAD = 3
LATE_STEP = 3
THREE_FROM = 6
OWN, PAIR, ONE, ZERO, THREE = range(5)
SELF_UNIT = (OWN, OWN)
OWN_PAIR = (PAIR, OWN)
KINDS = 3
UNITS = (
    (((), (), ()), ((), (), ()),
     ((), ((THREE, OWN),), ((ONE, OWN), (ONE, PAIR))), ((), (), ())),
    (((SELF_UNIT,), (), ()), ((SELF_UNIT,), (), ()),
     ((SELF_UNIT,), ((ZERO, PAIR),), ((ZERO, PAIR),)), ((SELF_UNIT,), ((ZERO, PAIR),), ((ZERO, PAIR),))),
    (((), (), ()), ((), (), ()),
     ((), ((THREE, PAIR),), ((THREE, OWN),)), ((), (), ())),
    (((), (OWN_PAIR,), (OWN_PAIR,)),
     (((ZERO, OWN),), ((PAIR, ZERO), OWN_PAIR), ((PAIR, ZERO), OWN_PAIR)),
     ((OWN_PAIR,), ((ONE, OWN), (ONE, PAIR)), ((THREE, PAIR),)),
     (((ZERO, OWN), OWN_PAIR), ((ONE, PAIR),), ((ONE, PAIR),))),
)


def line_kernel(sizes, emb, ids, prior, owned, owned_ids, dest,
                run_out, rows_out, ids_out, ret,
                raw, nrm, idv, idt, acc, obuf, oid, prior_v, owned_v, number_v, dest_v,
                local_sem, in_sem, send_sem, recv_sem, block_recv, ids_send, ids_recv, ret_send, ret_recv,
                rows_send, rows_recv, oids_send, oids_recv, keep_sem, known_sem):
    n_grp, n_blk = sizes
    devices = n_grp * n_blk
    rows = emb.shape[1]
    ch = rows // CHUNKS
    part = ch // SPLIT
    g = lax.axis_index("grp")
    b = lax.axis_index("blk")
    flip = g % 2
    z = b // 2
    x = b % 2
    role = z + flip * (3 - 2 * z)
    partner = b + 1 - 2 * x
    me = g * n_blk + b

    def block_of(r):
        return 2 * (r + flip * (3 - 2 * r)) + x

    def to_device(step):
        place = step - 1 + jnp.where(step > 2 * n_blk, 1, 0)
        turn = place // n_blk
        u = place % n_blk
        og = (g + u // 2) % n_grp
        oz = pick(4 * z + turn, [3, 2, 0, 1, 3, 2, 1, 0, 0, 1, 2, 3, 0, 1, 3, 2])
        ob = 2 * oz + (x + u) % 2
        return og * n_blk + ob, og, ob

    barrier = pltpu.get_barrier_semaphore()

    def signal(semaphore, grp, blk):
        pl.semaphore_signal(semaphore, inc=1, device_id=(grp, blk), device_id_type=pl.DeviceIdType.MESH)

    other_core = g + 1 - 2 * flip
    other_row = (g + n_grp // 2) % n_grp
    signal(barrier, g, partner)
    signal(barrier, other_core, b)
    signal(barrier, other_row, b)

    @pl.when(z > 0)
    def _():
        signal(barrier, g, b - 2)

    @pl.when(z < 3)
    def _():
        signal(barrier, g, b + 2)

    local = pltpu.make_async_copy(emb.at[0], raw.at[OWN], local_sem)
    local.start()
    inputs = [pltpu.make_async_copy(src, dst, in_sem.at[i]) for i, (src, dst) in enumerate((
        (ids, idv.at[OWN]), (prior, prior_v), (owned, owned_v), (owned_ids, number_v), (dest, dest_v)))]
    for copy in inputs:
        copy.start()

    pl.semaphore_wait(barrier, jnp.where((z == 1) | (z == 2), 5, 4))

    def told(here, index, then=None):
        @pl.when(here)
        def _():
            if index is not None:
                pl.semaphore_wait(known_sem.at[index], 1)
            if then is not None:
                signal(known_sem.at[then[0]], then[1], then[2])

    told(z == 0, None, (0, g, b + 2))
    told(z == 3, None, (1, g, b - 2))

    def remote(src, dst, ssem, rsem, blk, grp=None):
        return pltpu.make_async_remote_copy(
            src_ref=src, dst_ref=dst, send_sem=ssem, recv_sem=rsem,
            device_id=(g if grp is None else grp, blk), device_id_type=pl.DeviceIdType.MESH)

    def piece(k):
        if isinstance(k, int):
            return pl.ds(k * part, part)
        return pl.ds(pl.multiple_of(k * part, part), part)

    def span(c):
        if isinstance(c, int):
            return pl.ds(c * ch, ch)
        return pl.ds(pl.multiple_of(c * ch, ch), ch)

    whole = pl.ds(0, rows)
    pieces = SPLIT * CHUNKS

    own_slot = pick(role, [ZERO, ONE, ONE, THREE])
    own_to = block_of(pick(role, [1, 2, 3, 2]))
    has_own = role != 2
    onward = block_of(role + 1)
    gives_pair = (role > 0) | (x == 0)
    takes_pair = (role > 0) | (x == 1)
    early = role >= 2

    def own_copy(k, sem):
        return remote(emb.at[0, piece(k), :], raw.at[own_slot, piece(k), :],
                      send_sem.at[0, k // SPLIT], sem, own_to)

    def pair_copy(k):
        return remote(emb.at[0, piece(k), :], raw.at[PAIR, piece(k), :],
                      send_sem.at[1, k // SPLIT], block_recv.at[0, k // SPLIT], partner)

    def onward_copy(s, k):
        return remote(raw.at[s, piece(k), :], raw.at[s, piece(k), :],
                      send_sem.at[s, k // SPLIT], recv_sem.at[s - ONE, k], onward)

    def sent(lane, c):
        remote(raw.at[OWN, span(c), :], raw.at[OWN, span(c), :], send_sem.at[lane, c], block_recv.at[0, c], partner).wait_send()

    def send_own(first, last):
        @pl.when(role < 2)
        def _():
            for k in range(first, last):
                own_copy(k, recv_sem.at[own_slot - ONE, k]).start()

    def ids_copy(src, lane, slot, blk):
        return remote(src, idv.at[slot], ids_send.at[lane], ids_recv.at[slot], blk)

    @pl.when(has_own)
    def _():
        ids_copy(ids, 0, own_slot, own_to).start()

    send_own(0, SPLIT)

    @pl.when(role == 0)
    def _():
        send_own(SPLIT, pieces)

    @pl.when(gives_pair)
    def _():
        ids_copy(ids, 1, PAIR, partner).start()

    @pl.when(early)
    def _():
        for k in range(pieces):
            pair_copy(k).start()

    def normalize(values):
        values = values.astype(jnp.float32)
        scale = lax.rsqrt(jnp.sum(values * values, axis=-1, keepdims=True) + 1e-06)
        return (values * scale).astype(jnp.bfloat16)

    def ready(s, c):
        at = span(c)
        nrm[s, at, :] = normalize(raw[s, at, :])
        for p in range(ch // LANES):
            at = pl.ds(pl.multiple_of(c * ch + p * LANES, LANES), LANES)
            line = idv[s, :, at].astype(jnp.float32)
            idt[s, at, :] = jnp.transpose(jnp.broadcast_to(line, (LANES, LANES)))

    def tile(row, row_at, width, col, col_at):
        scores = lax.dot_general(
            nrm[col, col_at, :], nrm[row, row_at, :], (((1,), (1,)), ((), ())),
            preferred_element_type=jnp.float32)
        row_ids = idv[row, :, row_at].astype(jnp.float32)
        col_ids = idt[col, col_at, :]
        parts = []
        for p in range(width // LANES):
            cut = slice(p * LANES, (p + 1) * LANES)
            masked = jnp.where(col_ids < row_ids[:, cut], scores[:, cut], EMPTY)
            parts.append(jnp.max(masked, axis=0, keepdims=True))
        acc[row, :, row_at] = jnp.maximum(acc[row, :, row_at], jnp.concatenate(parts, axis=1))

    for s in range(1, 5):
        acc[s] = jnp.full((1, rows), EMPTY, jnp.float32)
    for copy in inputs:
        copy.wait()
    acc[OWN] = prior_v[...]
    local.wait()

    @pl.loop(0, CHUNKS)
    def _(c):
        ready(OWN, c)

    told(z == 1, 0, (0, g, b + 2))
    told(z == 2, 1, (1, g, b - 2))

    own_dev = owned.shape[0]
    owned_normed = normalize(owned_v[...])
    t_row = dest_v[...].astype(jnp.float32)
    t_col = jnp.transpose(jnp.broadcast_to(t_row, (LANES, own_dev)))[:, 0:1]
    row_i = lax.broadcasted_iota(jnp.int32, (own_dev, own_dev), 0)
    col_i = lax.broadcasted_iota(jnp.int32, (own_dev, own_dev), 1)
    earlier = jnp.where((row_i < col_i) & (t_col == t_row), 1.0, 0.0)
    position = jnp.sum(earlier, axis=0, keepdims=True)
    place = t_row * CAP + position
    which = lax.broadcasted_iota(jnp.int32, (devices * CAP, own_dev), 0).astype(jnp.float32)
    onehot = jnp.where(which == place, 1.0, 0.0).astype(jnp.bfloat16)
    outgoing = jnp.dot(onehot, owned_normed, preferred_element_type=jnp.float32).astype(jnp.bfloat16)
    dev_i = lax.broadcasted_iota(jnp.int32, (devices, own_dev), 0).astype(jnp.float32)
    lane_i = lax.broadcasted_iota(jnp.int32, (devices, LANES), 1)
    number = number_v[...].astype(jnp.float32) + 1.0
    outgoing_ids = jnp.full((devices, LANES), -1.0, jnp.float32)
    for k in range(CAP):
        here = jnp.where((dev_i == t_row) & (position == float(k)), number, 0.0)
        found = jnp.sum(here, axis=1, keepdims=True) - 1.0
        outgoing_ids = jnp.where(lane_i % CAP == k, found, outgoing_ids)
    outgoing_ids = outgoing_ids.astype(jnp.int32)
    for d in range(devices):
        obuf[d] = outgoing[d * CAP:(d + 1) * CAP, :]
        oid[d] = outgoing_ids[d:d + 1, :]

    told(z == 2, 0, (0, g, b + 2))
    told(z == 1, 1, (1, g, b - 2))

    keep_rows = pltpu.make_async_copy(obuf.at[me], rows_out.at[me], keep_sem.at[0])
    keep_ids = pltpu.make_async_copy(oid.at[me], ids_out.at[me], keep_sem.at[1])

    def start_routing(upward):
        @pl.loop(1, devices)
        def _(step):
            other, og, ob = to_device(step)

            @pl.when((ob // 2 > z) == upward)
            def _():
                remote(obuf.at[other], rows_out.at[me], rows_send, rows_recv, ob, og).start()
                remote(oid.at[other], ids_out.at[me], oids_send, oids_recv, ob, og).start()

        if not upward:
            keep_rows.start()
            keep_ids.start()

    def is_row(u, v):
        diff = (u - v + n_blk) % n_blk
        return (diff >= 1) & (diff <= CYCLE)

    slot_blocks = [b, partner, block_of(1), block_of(0), block_of(3)]

    def block_in(slot):
        result = slot_blocks[0]
        for i in range(1, 5):
            result = jnp.where(slot == i, slot_blocks[i], result)
        return result

    def run_units(table, kind, c):
        longest = max(len(entry) for by_phase in table for entry in by_phase)
        lists = [entry for by_phase in table for entry in by_phase]
        which_list = role * KINDS + kind
        ends = [int(len(entry) > 0 and entry[-1] == OWN_PAIR) for entry in lists]
        count = pick(which_list, [len(entry) for entry in lists]) - pick(which_list, ends) * (1 - x)

        @pl.loop(0, count)
        def _(j):
            def entry(i):
                return pick(j * len(lists) + which_list,
                            [(lst[n] if n < len(lst) else (0, 0))[i] for n in range(longest) for lst in lists])

            u, v = entry(0), entry(1)
            bu, bv = block_in(u), block_in(v)

            @pl.when(is_row(bv, bu) | (u == v))
            def _():
                tile(v, whole, rows, u, span(c))

            @pl.when(is_row(bu, bv))
            def _():
                tile(u, span(c), ch, v, whole)

    def ids_wait(s):
        ids_copy(idv.at[s], 1, s, partner).wait_recv()

    def stream_wait(s, k):
        remote(raw.at[s, piece(k), :], raw.at[s, piece(k), :], send_sem.at[1, 0], recv_sem.at[s - ONE, k], partner).wait_recv()

    def block_wait(s, c):
        remote(raw.at[s, span(c), :], raw.at[s, span(c), :], send_sem.at[1, 0],
               block_recv.at[int(s == THREE), c], partner).wait_recv()

    def back(slot, index, r):
        return remote(acc.at[slot], ret.at[index], ret_send.at[slot], ret_recv.at[index],
                      partner if r is None else block_of(r))

    def pass_on(s, k):
        stream_wait(s, k)

        @pl.when(role < 3)
        def _():
            onward_copy(s, k).start()

    def pass_ids(s):
        ids_wait(s)

        @pl.when(role < 3)
        def _():
            ids_copy(idv.at[s], s, s, onward).start()

    def take_three(c):
        @pl.when(c == 0)
        def _():
            ids_wait(THREE)

        block_wait(THREE, c)
        ready(THREE, c)

    @pl.when(role == 2)
    def _():
        pass_ids(ONE)
        for k in range(SPLIT):
            pass_on(ONE, k)
        ready(ONE, jnp.int32(0))

    @pl.loop(0, 2 * CHUNKS)
    def _(p):
        phase = p // CHUNKS
        c = p % CHUNKS
        has_in = (role > 0) & ((phase == 0) | (role > 1))
        s_in = jnp.where(phase == 0, ZERO, ONE)
        ahead = jnp.where((role == 2) & (phase == 1), 1, 0)
        c_in = (c + ahead) % CHUNKS
        last = p == 2 * CHUNKS - 1
        kind = phase + jnp.where(last, 1, 0)

        def take(i):
            k = SPLIT * c_in + i

            if i == 0:
                @pl.when(has_in & (c == 0) & ((role != 2) | (phase == 0)))
                def _():
                    pass_ids(s_in)

            @pl.when(has_in & (c + ahead < CHUNKS))
            def _():
                pass_on(s_in, k)

            if i == SPLIT - 1:
                @pl.when((phase == 0) & (role == 0))
                def _():
                    sent(0, c)

            @pl.when((phase == 0) & (role == 3) & (k >= THREE_FROM) & (k < THREE_FROM + pieces // 2))
            def _():
                for n in range(2):
                    m = 2 * (k - THREE_FROM) + n
                    own_copy(m, block_recv.at[1, m // SPLIT]).start()

        @pl.when((phase == 1) & (role == 0) & gives_pair & (c > 0))
        def _():
            sent(1, c - 1)

        @pl.when((phase == 1) & (role < 2) & gives_pair & (c + LATE_LEAD < CHUNKS))
        def _():
            for i in range(SPLIT):
                pair_copy(SPLIT * (c + LATE_LEAD) + i).start()

        take(0)

        @pl.when((p == 2 * CHUNKS - 1) & (role == 3))
        def _():
            start_routing(False)

        @pl.when((role == 2) & (phase == 1))
        def _():
            take_three(c)

        run_units(UNITS[0], kind, jnp.where(last, c_in, c))

        @pl.when(last & (role == 2))
        def _():
            back(ONE, 2, 1).start()

        take(1)

        @pl.when((p == LATE_STEP) & (role < 2) & gives_pair)
        def _():
            for k in range(LATE_LEAD * SPLIT):
                pair_copy(k).start()

        run_units(UNITS[1], kind, c)

        @pl.when((p == 2 * CHUNKS - 1) & early)
        def _():
            back(ZERO, role, 0).start()
            start_routing(True)

        take(2)
        run_units(UNITS[2], kind, c)
        take(3)

        @pl.when((phase == 1) & (role < 2) & takes_pair)
        def _():
            @pl.when(c == 0)
            def _():
                ids_wait(PAIR)

            block_wait(PAIR, c)

        @pl.when((p == 2 * CHUNKS - 1) & (role == 0) & gives_pair)
        def _():
            sent(1, c)

        @pl.when((role < 3) & (p == jnp.where(role == 2, 2 * CHUNKS - 2, 2 * CHUNKS - 1)))
        def _():
            start_routing(False)

        @pl.when((p == CHUNKS - 1) & (role == 1))
        def _():
            send_own(SPLIT, pieces)

        told((p == 0) & (z == 3), 0)
        told((p == 0) & (z == 0), 1)
        told(p == 1, None, (2, other_core, b))
        told(p == 3, 2, (3, other_row, b))
        told(p == 4, 3)

        @pl.when(has_in & (c + ahead < CHUNKS))
        def _():
            ready(s_in, c_in)

        @pl.when((phase == 0) & early)
        def _():
            @pl.when(c == 0)
            def _():
                ids_wait(PAIR)

            block_wait(PAIR, c)

        @pl.when((early == (phase == 0)) & takes_pair)
        def _():
            ready(PAIR, c)

        run_units(UNITS[3], kind, jnp.where(last, c, c_in))

    returns = [(role > 0, PAIR, 0, None), (role == 1, ZERO, 1, 0), (role == 2, ZERO, 2, 0), (role == 3, ZERO, 3, 0),
               (role == 2, ONE, 2, 1), (role == 3, ONE, 3, 1), (role == 2, THREE, 2, 3)]
    for when, slot, index, r in reversed(returns):
        if (slot == ZERO and index > 1) or (slot, index) == (ONE, 2):
            continue

        @pl.when(when)
        def _(slot=slot, index=index, r=r):
            back(slot, index, r).start()

    def returned(index):
        remote(acc.at[PAIR], ret.at[index], ret_send.at[PAIR], ret_recv.at[index], partner).wait_recv()

    @pl.when(role < 2)
    def _():
        start_routing(True)

    own_result = pltpu.make_async_copy(acc.at[OWN], run_out, keep_sem.at[2])
    own_result.start()

    @pl.when(gives_pair)
    def _():
        ids_copy(ids, 1, PAIR, partner).wait_send()

    @pl.when(role > 0)
    def _():
        for c in range(CHUNKS):
            sent(1, c)

    @pl.when(has_own)
    def _():
        ids_copy(ids, 0, own_slot, own_to).wait_send()

    @pl.when((role == 1) | (role == 3))
    def _():
        for c in range(CHUNKS):
            sent(0, c)

    for s, sends in ((ONE, role == 2), (ZERO, (role == 1) | (role == 2))):
        @pl.when(sends)
        def _(s=s):
            ids_copy(idv.at[s], s, s, onward).wait_send()
            for c in range(CHUNKS):
                sent(s, c)

    own_result.wait()
    keep_rows.wait()
    keep_ids.wait()
    others = pl.ds(0, devices - 1)
    pltpu.make_async_copy(obuf.at[others], rows_out.at[others], rows_send).wait()
    pltpu.make_async_copy(oid.at[others], ids_out.at[others], oids_send).wait()
    pltpu.make_async_copy(obuf.at[others], rows_out.at[others], rows_recv).wait()
    pltpu.make_async_copy(oid.at[others], ids_out.at[others], oids_recv).wait()

    for index, gets in ((0, role > 0), (1, role == 0), (2, role != 2), (3, role < 2)):
        @pl.when(gets)
        def _(index=index):
            returned(index)

    for when, slot, index, r in returns:
        @pl.when(when)
        def _(slot=slot, index=index, r=r):
            back(slot, index, r).wait_send()


def place_kernel(line, run, routed, routed_ids, *rest):
    if line:
        ret, run_out, rows_out, ids_out = rest
        z = lax.axis_index("blk") // 2
        role = z + (lax.axis_index("grp") % 2) * (3 - 2 * z)
        result = run[...]
        for index, gets in enumerate((role > 0, role == 0, role != 2, role < 2)):
            result = jnp.maximum(result, jnp.where(gets, ret[index], EMPTY))
        run_out[...] = result
    else:
        run_out, rows_out, ids_out = rest
        run_out[...] = run[...]
    devices, cap, _ = routed.shape
    for d in range(0, devices, 2):
        both = jnp.concatenate([routed[d].astype(jnp.float32), routed[d + 1].astype(jnp.float32)], axis=0)
        rows_out[d * cap:(d + 2) * cap, :] = both.astype(jnp.bfloat16)
    lines = routed_ids[...].reshape(devices, LANES)
    for part in range(devices * cap // LANES):
        sub = lines[part * LANES // cap:(part + 1) * LANES // cap, :]
        row_i = lax.broadcasted_iota(jnp.int32, sub.shape, 0)
        lane_i = lax.broadcasted_iota(jnp.int32, sub.shape, 1)
        mine = jnp.where(lane_i // cap == row_i, sub, 0)
        ids_out[:, part * LANES:(part + 1) * LANES] = jnp.sum(mine, axis=0, keepdims=True)


def body(embeds, doc_ids, prior_max, owned, owned_ids, owner_dest):
    n_grp, n_blk = lax.axis_size("grp"), lax.axis_size("blk")
    devices = n_grp * n_blk
    line = (n_grp, n_blk) == (4, 8)
    rows, width = embeds.shape[1:]
    own_dev = owned.shape[0]
    vmem = pl.BlockSpec(memory_space=pltpu.VMEM)
    anywhere = pl.BlockSpec(memory_space=pl.ANY)
    dma = pltpu.SemaphoreType.DMA
    shapes = (
        jax.ShapeDtypeStruct((1, rows), jnp.float32),
        jax.ShapeDtypeStruct((devices, CAP, width), jnp.bfloat16),
        jax.ShapeDtypeStruct((devices, 1, LANES), jnp.int32),
    )
    limit = 60 * 1024 * 1024
    if line:
        slots, pieces = 5, SPLIT * CHUNKS
        results = pl.pallas_call(
            functools.partial(line_kernel, (n_grp, n_blk)),
            out_shape=shapes + (jax.ShapeDtypeStruct((4, 1, rows), jnp.float32),),
            in_specs=[anywhere] * 6,
            out_specs=(anywhere,) * 4,
            scratch_shapes=[
                pltpu.VMEM((slots, rows, width), jnp.bfloat16),
                pltpu.VMEM((slots, rows, width), jnp.bfloat16),
                pltpu.VMEM((slots, 1, rows), jnp.int32),
                pltpu.VMEM((slots, rows, LANES), jnp.float32),
                pltpu.VMEM((slots, 1, rows), jnp.float32),
                pltpu.VMEM((devices, CAP, width), jnp.bfloat16),
                pltpu.VMEM((devices, 1, LANES), jnp.int32),
                pltpu.VMEM((1, rows), jnp.float32),
                pltpu.VMEM((own_dev, width), jnp.bfloat16),
                pltpu.VMEM((1, own_dev), jnp.int32),
                pltpu.VMEM((1, own_dev), jnp.int32),
                dma, dma((5,)), dma((4, CHUNKS)), dma((2, pieces)), dma((2, CHUNKS)),
                dma((slots,)), dma((slots,)), dma((slots,)), dma((4,)),
                dma, dma, dma, dma, dma((3,)), pltpu.SemaphoreType.REGULAR((4,)),
            ],
            compiler_params=pltpu.CompilerParams(has_side_effects=True, collective_id=0, vmem_limit_bytes=limit),
        )(embeds, doc_ids, prior_max, owned, owned_ids.reshape(1, own_dev), owner_dest.reshape(1, own_dev))
    else:
        plan = make_plan(n_blk // 2)
        received, returns = plan[0], plan[5]
        slots = max(len(entry) for entry in received)
        results = pl.pallas_call(
            functools.partial(ring_kernel, plan, (n_grp, n_blk)),
            out_shape=shapes,
            in_specs=[anywhere, vmem, vmem, vmem, vmem, vmem],
            out_specs=(vmem, anywhere, anywhere),
            scratch_shapes=[
                pltpu.VMEM((2 + slots, rows, width), jnp.bfloat16),
                pltpu.VMEM((2 + slots, rows, width), jnp.bfloat16),
                pltpu.VMEM((2 + slots, 1, rows), jnp.int32),
                pltpu.VMEM((2 + slots, rows, LANES), jnp.float32),
                pltpu.VMEM((2 + slots, 1, rows), jnp.float32),
                pltpu.VMEM((1 + max(returns), 1, rows), jnp.float32),
                pltpu.VMEM((devices, CAP, width), jnp.bfloat16),
                pltpu.VMEM((devices, 1, LANES), jnp.int32),
                dma, dma((2 + slots, CHUNKS)), dma((2 + slots, CHUNKS)),
                dma((2 + slots,)), dma((2 + slots,)),
                dma((1 + slots,)), dma((1 + max(returns),)),
                dma, dma, dma, dma, dma((2,)),
            ],
            compiler_params=pltpu.CompilerParams(has_side_effects=True, vmem_limit_bytes=limit),
        )(embeds, doc_ids, prior_max, owned, owned_ids.reshape(1, own_dev), owner_dest)
    running, next_rows, next_ids = pl.pallas_call(
        functools.partial(place_kernel, line),
        out_shape=(
            jax.ShapeDtypeStruct((1, rows), jnp.float32),
            jax.ShapeDtypeStruct((devices * CAP, width), jnp.bfloat16),
            jax.ShapeDtypeStruct((1, devices * CAP), jnp.int32),
        ),
        in_specs=[vmem] * len(results),
        out_specs=(vmem,) * 3,
    )(*results)
    return (running, next_rows, next_ids.reshape(devices * CAP))


def solution(mesh):
    return jax.shard_map(
        body,
        mesh=mesh,
        in_specs=(
            P("grp", "blk", None),
            P("grp", "blk"),
            P("grp", "blk"),
            P(("grp", "blk"), None),
            P(("grp", "blk")),
            P(("grp", "blk"), None),
        ),
        out_specs=(P("grp", "blk"), P(("grp", "blk"), None), P(("grp", "blk"))),
        check_vma=False,
    )
```
